512 devices in a mesh: gx: 4 (over x), gy: 8 (over z), gz: 16 (over y, core).
Axes of the slice: x: 4, y: 8, z: 8, core: 2. Of those that a mesh axis runs over, the one named last changes fastest.
Arguments:
- positions: float32 [3, 262144], P(None, ('gx', 'gy', 'gz')), may hold values from -6 to 6
- frames: float32 [128, 3, 4096], P(None, None, ('gy', 'gz')), may hold values from -6 to 6
- path_slot: int32 [512, 32], P(('gx', 'gy', 'gz')), may hold values from 0 to 511, as said below
- path_count: int32 [512], replicated, may hold values from 1 to 32, 4096 in all
- path_order: int32 [4096], replicated, may hold values from 0 to 4095, each once
- frame_rank: int32 [128], replicated, may hold values from 0 to 127, each once
Outputs:
- forces: float32 [3, 262144], P(None, ('gx', 'gy', 'gz'))
- path_cv: float32 [2], replicated
The draws below stay inside these ranges and needn't reach their ends.
Inputs may be any that keep to these rules, and one draw needn't show every extreme that they name: `path_slot`: within one domain's row the 32 local atom indices are all different.
All inputs are finite; a program needn't handle non-finite values.
Results may differ from the reference program's by a relative error of at most 0.00013.
Values sent between devices are 32-bit elements; how exact they have to be, the bound alone decides.
No kernel may reach another device: no remote copies, remote signals or barrier semaphores. Data moves between devices by JAX's collectives and lax.ppermute only.
A program may use at most 64 MiB of HBM per device.

```python
import math
import jax
import jax.numpy as jnp
import numpy as np
from jax import lax

P_SIZE = 4096
F = 128
ATOM_DEV = 512
SLOTS = 32
ATOMS = 262144
DEVICES = 512


def draw_path_slot(key, part):
    keys = jax.random.split(jax.random.fold_in(key, 17), DEVICES)
    rows = jax.vmap(lambda k: jax.random.permutation(k, ATOM_DEV)[:SLOTS])(keys)
    return rows.astype(jnp.int32)


def levels(rng, extent, cuts, low, largest):
    gain, own = 1.0, jax.random.fold_in(rng, 6)
    for dim, blocks in cuts:
        steps = jnp.exp(jax.random.uniform(jax.random.fold_in(own, dim), (blocks,), jnp.float32, low / len(cuts), largest / len(cuts)))
        gain = gain * jnp.repeat(steps, extent[dim] // blocks).reshape([-1 if axis == dim else 1 for axis in range(len(extent))])
    return gain


def split_up(amount, total, limit, lean):
    loads = [(1 << 20) // math.isqrt(grade ** lean) + 1 for grade in range(2, amount + 1)]
    rest, counts = total - limit - (amount - 1), [1] * (amount - 1)
    while rest > 0:
        free = [i for i in range(amount - 1) if counts[i] < limit]
        whole, remaining = sum([loads[i] for i in free]), rest
        for i in free:
            more = min(limit - counts[i], max(1, remaining * loads[i] // whole), rest)
            counts[i] = counts[i] + more
            rest = rest - more
    return np.array([limit] + counts)


def ragged(stream_key, number_of, total, most, slope):
    if number_of == 2:
        one = jax.random.randint(stream_key, (), max(1, total - most), min(most, total - 1) + 1)
        return jnp.stack([one, total - one])
    tallies = jnp.asarray(split_up(number_of, total, most, slope), jnp.int32)
    couples = (number_of - 1) // 2
    source_of, taker = tallies[1:1 + 2 * couples:2], tallies[2:2 + 2 * couples:2]
    room = jnp.minimum(source_of - 1, most - taker)
    shifted = jax.random.randint(jax.random.fold_in(stream_key, 1), (couples,), 0, 1 << 20) % (room + 1)
    tallies = tallies.at[1:1 + 2 * couples:2].set(source_of - shifted).at[2:2 + 2 * couples:2].set(taker + shifted)
    return tallies[jax.random.permutation(jax.random.fold_in(stream_key, 2), number_of)]


def centred(stream_key, shape, scale, reach, pieces=(), kind=jnp.bfloat16):
    gain = levels(stream_key, shape, pieces, -0.22, 0.18) if pieces else 1.0
    array = jax.random.normal(stream_key, shape, jnp.float32) * scale * gain
    return jnp.minimum(jnp.maximum(array, -reach), reach).astype(kind)


def setup_inputs(seed: int = 0) -> dict:
    arg_keys = jax.random.split(jax.random.key(seed), 7)
    return {
        "positions": centred(arg_keys[0], (3, ATOMS), 1.0, 6.0, ((1, 512),), jnp.float32),
        "frames": centred(arg_keys[1], (F, 3, P_SIZE), 1.0, 6.0, ((2, 128),), jnp.float32),
        "path_slot": draw_path_slot(jax.random.fold_in(arg_keys[6], 71), 0),
        "path_count": ragged(arg_keys[3], DEVICES, P_SIZE, SLOTS, 2).astype(jnp.int32),
        "path_order": jax.random.permutation(arg_keys[4], P_SIZE).astype(jnp.int32),
        "frame_rank": jax.random.permutation(arg_keys[5], F).astype(jnp.int32),
    }


STRENGTH = 20.0
S_HOME = 0.5
KAPPA_S = 0.5
KAPPA_Z = 0.05
PAIR_SCALE = 0.02
WIDTH_SQ = 4.0


def pair_block(block_pos, all_pos):
    diff = block_pos[:, :, None] - all_pos[:, None, :]
    dist_sq = jnp.sum(diff * diff, axis=0)
    weight = PAIR_SCALE * jnp.exp(-dist_sq / WIDTH_SQ)
    return jnp.sum(weight[None] * diff, axis=2)


def domain_forces(local):
    atoms = local.shape[1]
    rows = 256 if atoms % 256 == 0 else atoms
    blocks = local.reshape(3, atoms // rows, rows).transpose(1, 0, 2)
    result = lax.map(lambda block: pair_block(block, local), blocks)
    return result.transpose(1, 0, 2).reshape(3, atoms)


def slot_ids(path_count, path_order, slots):
    offsets = jnp.cumsum(path_count) - path_count
    steps_k = jnp.arange(slots, dtype=jnp.int32)
    live = steps_k[None, :] < path_count[:, None]
    place = jnp.clip(offsets[:, None] + steps_k[None, :], 0, P_SIZE - 1).astype(jnp.int32)
    ids = jnp.where(live, path_order[place], -1).astype(jnp.int32)
    return ids, live


def cv_terms(dist, frame_rank):
    frames_n = dist.shape[0]
    expo = -STRENGTH * dist
    top = jnp.max(expo)
    expd = jnp.exp(expo - top)
    total = jnp.sum(expd)
    weight = expd / total
    progress_rank = frame_rank.astype(jnp.float32) / (frames_n - 1.0)
    s_value = jnp.sum(progress_rank * weight)
    z_value = -(top + jnp.log(total)) / STRENGTH
    grads = KAPPA_S * P_SIZE * (s_value - S_HOME) * (-STRENGTH) * weight * (progress_rank - s_value) + KAPPA_Z * P_SIZE * z_value * weight
    return s_value, z_value, grads


def reference(positions, frames, path_slot, path_count, path_order, frame_rank):
    domains = path_slot.shape[0]
    slots = path_slot.shape[1]
    ids, live = slot_ids(path_count, path_order, slots)
    atom_index = (jnp.arange(domains, dtype=jnp.int32)[:, None] * ATOM_DEV + path_slot).astype(jnp.int32)
    flat_atoms = atom_index.reshape(-1)
    flat_ids = jnp.clip(ids.reshape(-1), 0, P_SIZE - 1).astype(jnp.int32)
    mask = live.reshape(-1).astype(jnp.float32)
    path_pos = positions[:, flat_atoms]
    refs = frames[:, :, flat_ids]
    delta = path_pos[None] - refs
    dist = jnp.sum(jnp.sum(delta * delta, axis=1) * mask[None], axis=1) / P_SIZE
    s_value, z_value, grads = cv_terms(dist, frame_rank)
    bias = -(2.0 / P_SIZE) * jnp.einsum('f,fcm->cm', grads, delta, precision=lax.Precision.HIGHEST) * mask[None]
    local = positions.reshape(3, domains, ATOM_DEV).transpose(1, 0, 2)
    pair = lax.map(domain_forces, local)
    forces = pair.transpose(1, 0, 2).reshape(3, domains * ATOM_DEV)
    forces = forces.at[:, flat_atoms].add(bias)
    return forces, jnp.stack([s_value, z_value])
```

```python
import functools

import jax
import jax.numpy as jnp
from jax import lax
from jax.experimental import pallas as pl
from jax.experimental.pallas import tpu as pltpu
from jax.sharding import Mesh
from jax.sharding import PartitionSpec as P

P_SIZE = 4096
F = 128
ATOMS_LOCAL = 512
SLOTS = 32
LANES = 128
BLOCK = 32

ALL = ("gx", "gy", "gz_0", "gz_1")
HOLDERS = ("gy", "gz_0", "gz_1")
CHIPS = ("gy", "gz_0")
ROWS = ("gx", "gz_1")
N_CHIPS = 64
N_ROWS = 8
IDS = 2 * BLOCK

STRENGTH = 20.0
S_HOME = 0.5
KAPPA_S = 0.5
KAPPA_Z = 0.05
PAIR_SCALE = 0.02
WIDTH_SQ = 4.0

HIGHEST = lax.Precision.HIGHEST
F32 = jnp.float32
I32 = jnp.int32
VMEM = pl.BlockSpec(memory_space=pltpu.VMEM)


def holder_index():
    return lax.axis_index("gy") * 16 + lax.axis_index("gz_0") * 2 + lax.axis_index("gz_1")


def iota(shape, dim):
    return lax.broadcasted_iota(I32, shape, dim)


def call(kernel, out_shape, name, inputs, scratch=()):
    return pl.pallas_call(
        kernel,
        out_shape=out_shape,
        in_specs=[VMEM] * len(inputs),
        out_specs=jax.tree.map(lambda _: VMEM, out_shape),
        scratch_shapes=scratch,
        name=name,
        compiler_params=pltpu.CompilerParams(vmem_limit_bytes=8 << 20),
        cost_estimate=pl.CostEstimate(flops=2000000, bytes_accessed=100000, transcendentals=0),
    )(*inputs)


def pack_kernel(count_ref, order_ref, slot_ref, pos_ref, out_ref, ids_ref):
    here = lax.axis_index("gx") * 128 + holder_index()
    counts = count_ref[...]
    domain = iota(counts.shape, 0) * LANES + iota(counts.shape, 1)
    offset = jnp.sum(jnp.where(domain < here, counts, 0))
    mine = jnp.sum(jnp.where(domain == here, counts, 0))
    row = offset // LANES
    shift = offset - row * LANES
    first = order_ref[pl.ds(row, 1), :]
    second = order_ref[pl.ds(jnp.minimum(row + 1, P_SIZE // LANES - 1), 1), :]
    lane = iota((1, LANES), 1)
    k = lane & (SLOTS - 1)
    turn = jnp.where(shift == 0, 0, LANES - shift)
    ids = jnp.where(lane < LANES - shift, pltpu.roll(first, turn, 1), pltpu.roll(second, turn, 1))
    ids = jnp.where(lane < SLOTS, ids, 0)
    slots = jnp.concatenate([slot_ref[...]] * 4, axis=1)
    ids = ids + pltpu.roll(ids, 2 * SLOTS, 1)
    ids = ids + pltpu.roll(ids, SLOTS, 1)
    live = k < mine
    ids = jnp.where(live, ids, -1)
    ids_ref[...] = ids
    pick = (iota((ATOMS_LOCAL, LANES), 0) == slots).astype(F32)
    xyz = jnp.dot(pos_ref[...], pick, precision=HIGHEST, preferred_element_type=F32)
    part = lane // SLOTS
    row_out = jnp.where(part == 0, xyz[0:1], jnp.where(part == 1, xyz[1:2], xyz[2:3]))
    row_out = jnp.where(live, row_out, 0.0)
    row_out = jnp.where(part == 3, ids.astype(F32), row_out)
    out_ref[...] = jnp.broadcast_to(row_out, out_ref.shape)


def dist_kernel(got_ref, mine_ref, other_ref, out_ref, coded):
    holder = holder_index()
    chip, core = holder // 2, holder & 1
    got = got_ref[...]
    lane = iota(got.shape, 1)
    part = lane // SLOTS
    ids = jnp.where(part == 3, got, 0.0)
    ids = ids + pltpu.roll(ids, 2 * SLOTS, 1)
    ids = ids + pltpu.roll(ids, SLOTS, 1)
    coded[0] = ids
    coded[1] = jnp.where(part == 3, 1.0, got)
    j = iota((IDS, LANES), 0)
    own = (chip * IDS + (j ^ (core * BLOCK))).astype(F32)
    found = jnp.zeros((IDS, LANES), F32)
    for m in range(N_CHIPS):
        found = found + jnp.where(coded[0, m : m + 1, :] == own, coded[1, m : m + 1, :], 0.0)
    part = iota((IDS, LANES), 1) // SLOTS
    column = [jnp.sum(jnp.where(part == c, found, 0.0), axis=1, keepdims=True) for c in range(4)]
    total = jnp.zeros((BLOCK, F), F32)
    for half, frames in ((0, mine_ref), (1, other_ref)):
        low = half * BLOCK
        square = jnp.zeros((BLOCK, F), F32)
        for c in range(3):
            delta = column[c][low : low + BLOCK] - frames[c * BLOCK : (c + 1) * BLOCK, :]
            square = square + delta * delta
        total = total + square * column[3][low : low + BLOCK]
    partial = jnp.sum(total, axis=0, keepdims=True) * (1.0 / P_SIZE)
    out_ref[...] = jnp.broadcast_to(partial, out_ref.shape)


def sum_kernel(got_ref, out_ref):
    out_ref[...] = jnp.broadcast_to(jnp.sum(got_ref[...], axis=0, keepdims=True), out_ref.shape)


def bias_kernel(got_ref, rank_ref, mine_ref, other_ref, out_ref, cv_ref):
    dist = jnp.sum(got_ref[...], axis=0, keepdims=True)
    expo = -STRENGTH * dist
    top = jnp.max(expo, axis=1, keepdims=True)
    expd = jnp.exp(expo - top)
    total = jnp.sum(expd, axis=1, keepdims=True)
    weight = expd / total
    rank = rank_ref[...].astype(F32) / (F - 1.0)
    s_value = jnp.sum(rank * weight, axis=1, keepdims=True)
    z_value = -(top + jnp.log(total)) / STRENGTH
    grads = (
        KAPPA_S * P_SIZE * (s_value - S_HOME) * -STRENGTH * weight * (rank - s_value)
        + KAPPA_Z * P_SIZE * z_value * weight
    )
    lane = iota((1, LANES), 1)
    cv_ref[...] = jnp.where(lane == 0, s_value, z_value)
    eight = jnp.broadcast_to(grads, (8, F))
    dims = (((1,), (1,)), ((), ()))
    own = lax.dot_general(eight, mine_ref[...], dims, precision=HIGHEST, preferred_element_type=F32)
    oth = lax.dot_general(eight, other_ref[...], dims, precision=HIGHEST, preferred_element_type=F32)
    whole = jnp.broadcast_to(jnp.sum(grads, axis=1, keepdims=True), (1, BLOCK))
    own = jnp.concatenate([own[0:1], whole], axis=1)
    oth = jnp.concatenate([oth[0:1], whole], axis=1)
    out_ref[...] = jnp.where((iota(out_ref.shape, 0) & 1) == 0, own, oth)


def pair_kernel(pos_ref, out_ref):
    pos = pos_ref[...]
    columns = jnp.transpose(jnp.concatenate([pos, pos[0:1]] * 2, axis=0))
    scale = -1.0 / (WIDTH_SQ * 0.6931471805599453)
    step = 64
    sums = [jnp.zeros((8, ATOMS_LOCAL), F32) for _ in range(3)]
    for i in range(0, ATOMS_LOCAL, step):
        diff = [pos[c : c + 1, :] - columns[i : i + step, c : c + 1] for c in range(3)]
        dist_sq = diff[0] * diff[0] + diff[1] * diff[1] + diff[2] * diff[2]
        weight = jnp.exp2(dist_sq * scale)
        for c in range(3):
            term = weight * diff[c]
            for r in range(0, step, 8):
                sums[c] = sums[c] + term[r : r + 8]
    for c in range(3):
        out_ref[c : c + 1, :] = PAIR_SCALE * jnp.sum(sums[c], axis=0, keepdims=True)


def force_kernel(got_ref, ids_ref, slot_ref, pos_ref, pair_ref, out_ref):
    core = lax.axis_index("gz_1")
    ids = ids_ref[:, 0:SLOTS]
    source = (ids // BLOCK) ^ core
    from_row = (iota((2 * N_CHIPS, SLOTS), 0) == source).astype(F32)
    dims = (((0,), (0,)), ((), ()))
    rows = lax.dot_general(got_ref[...], from_row, dims, precision=HIGHEST, preferred_element_type=F32)
    at = (iota((BLOCK, SLOTS), 0) == (ids & (BLOCK - 1))).astype(F32)
    slots = slot_ref[...]
    pick = (iota((ATOMS_LOCAL, SLOTS), 0) == slots).astype(F32)
    sums = [jnp.sum(rows[c * BLOCK : (c + 1) * BLOCK] * at, axis=0, keepdims=True) for c in range(3)]
    whole = rows[96:97]
    live = (ids >= 0).astype(F32)
    scattered = lax.dot_general(
        jnp.concatenate(sums + [whole] * 5, axis=0) * live,
        pick,
        (((1,), (1,)), ((), ())),
        precision=HIGHEST,
        preferred_element_type=F32,
    )
    bias = (-2.0 / P_SIZE) * (pos_ref[...] * scattered[3:4] - scattered[0:3])
    out_ref[...] = pair_ref[...] + bias


def shaped(*shape, dtype=F32):
    return jax.ShapeDtypeStruct(shape, dtype)


def spread(rows, axes):
    return lax.all_to_all(rows, axes, 0, 0, tiled=True)


def body(positions, frames, path_slot, path_count, path_order, frame_rank):
    mine = jnp.transpose(frames, (1, 2, 0)).reshape(3 * BLOCK, F)
    other = lax.ppermute(mine, "gz_1", [(0, 1), (1, 0)])
    sent, ids = call(
        pack_kernel,
        (shaped(N_CHIPS, LANES), shaped(1, LANES, dtype=I32)),
        "pack",
        (path_count.reshape(4, LANES), path_order.reshape(32, LANES), path_slot, positions),
    )
    pair = call(pair_kernel, shaped(3, ATOMS_LOCAL), "pair", (positions,))
    atoms = spread(sent, CHIPS)
    coded = [pltpu.VMEM((2, N_CHIPS, LANES), F32)]
    partial = call(dist_kernel, shaped(N_CHIPS, LANES), "dist", (atoms, mine, other), coded)
    over_chips = spread(partial, CHIPS)
    row_sum = call(sum_kernel, shaped(N_ROWS, LANES), "sum", (over_chips,))
    over_rows = spread(row_sum, ROWS)
    biases, cv = call(
        bias_kernel,
        (shaped(2 * N_CHIPS, LANES), shaped(1, LANES)),
        "bias",
        (over_rows, frame_rank.reshape(1, F), mine, other),
    )
    back = spread(biases, CHIPS)
    forces = call(
        force_kernel, shaped(3, ATOMS_LOCAL), "force", (back, ids, path_slot, positions, pair)
    )
    return forces, cv[0, 0:2]


def solution(mesh):
    finer = Mesh(mesh.devices.reshape(mesh.shape["gx"], mesh.shape["gy"], 8, 2), ALL)
    return jax.shard_map(
        body,
        mesh=finer,
        in_specs=(P(None, ALL), P(None, None, HOLDERS), P(ALL, None), P(), P(), P()),
        out_specs=(P(None, ALL), P()),
        check_vma=False,
    )
```

```python
import math

import jax
import jax.numpy as jnp
from jax import lax
from jax.experimental import pallas as pl
from jax.experimental.pallas import tpu as pltpu
from jax.sharding import Mesh
from jax.sharding import PartitionSpec as P

P_SIZE = 4096
F = 128
ATOMS_LOCAL = 512
SLOTS = 32
LANES = 128
BLOCK = 32

ALL = ("gx", "gy", "gz_0", "gz_1")
HOLDERS = ("gy", "gz_0", "gz_1")
N_HOLDERS = 128
FIRST = ("gx", "gy")
N_FIRST = 32
SECOND = ("gz_0", "gz_1")
N_SECOND = 16

STRENGTH = 20.0
S_HOME = 0.5
KAPPA_S = 0.5
KAPPA_Z = 0.05
PAIR_SCALE = 0.02
WIDTH_SQ = 4.0

HIGHEST = lax.Precision.HIGHEST
F32 = jnp.float32
I32 = jnp.int32
VMEM = pl.BlockSpec(memory_space=pltpu.VMEM)
HBM = pl.BlockSpec(memory_space=pltpu.HBM)


def holder_index():
    return lax.axis_index("gy") * 16 + lax.axis_index("gz_0") * 2 + lax.axis_index("gz_1")


def iota(shape, dim):
    return lax.broadcasted_iota(I32, shape, dim)


def shaped(*shape, dtype=F32):
    return jax.ShapeDtypeStruct(shape, dtype)


def call(kernel, out_shape, name, inputs, **kwargs):
    return pl.pallas_call(
        kernel,
        out_shape=out_shape,
        out_specs=jax.tree.map(lambda _: VMEM, out_shape),
        name=name,
        cost_estimate=pl.CostEstimate(flops=2000000, bytes_accessed=100000, transcendentals=0),
        **kwargs,
    )(*inputs)


def small(kernel, out_shape, name, inputs, scratch=()):
    return call(
        kernel,
        out_shape,
        name,
        inputs,
        in_specs=[VMEM] * len(inputs),
        scratch_shapes=scratch,
        compiler_params=pltpu.CompilerParams(vmem_limit_bytes=8 << 20),
    )


def pair_forces(pos, out_ref):
    columns = jnp.transpose(jnp.concatenate([pos, pos[0:1]] * 2, axis=0))
    scale = -1.0 / (WIDTH_SQ * math.log(2.0))
    step = 64
    sums = [jnp.zeros((8, ATOMS_LOCAL), F32) for _ in range(3)]
    for i in range(0, ATOMS_LOCAL, step):
        diff = [pos[c : c + 1, :] - columns[i : i + step, c : c + 1] for c in range(3)]
        dist_sq = diff[0] * diff[0] + diff[1] * diff[1] + diff[2] * diff[2]
        weight = jnp.exp2(dist_sq * scale)
        for c in range(3):
            term = weight * diff[c]
            for r in range(0, step, 8):
                sums[c] = sums[c] + term[r : r + 8]
    for c in range(3):
        out_ref[c : c + 1, :] = PAIR_SCALE * jnp.sum(sums[c], axis=0, keepdims=True)


def pack_kernel(
    count_hbm, order_hbm, slot_hbm, pos_hbm, rank_hbm, out_ref, aux_ref, xyz_ref, pair_ref, count_ref, order_ref, slot_ref, pos_ref, rank_ref, sems
):
    copies = [
        pltpu.make_async_copy(source, target, sems.at[i])
        for i, (source, target) in enumerate(
            (
                (count_hbm, count_ref),
                (order_hbm, order_ref),
                (slot_hbm, slot_ref),
                (pos_hbm, pos_ref),
                (rank_hbm, rank_ref),
            )
        )
    ]
    for copy in copies:
        copy.start()
    here = lax.axis_index("gx") * N_HOLDERS + holder_index()
    copies[0].wait()
    counts = count_ref[...]
    domain = iota(counts.shape, 0) * LANES + iota(counts.shape, 1)
    offset = jnp.sum(jnp.where(domain < here, counts, 0))
    mine = jnp.sum(jnp.where(domain == here, counts, 0))
    copies[1].wait()
    row = offset // LANES
    shift = offset - row * LANES
    first = order_ref[pl.ds(row, 1), :]
    second = order_ref[pl.ds(jnp.minimum(row + 1, P_SIZE // LANES - 1), 1), :]
    lane = iota((1, LANES), 1)
    k = lane & (SLOTS - 1)
    turn = jnp.where(shift == 0, 0, LANES - shift)
    ids = jnp.where(lane < LANES - shift, pltpu.roll(first, turn, 1), pltpu.roll(second, turn, 1))
    ids = jnp.where(lane < SLOTS, ids, 0)
    copies[2].wait()
    slots = jnp.concatenate([slot_ref[...]] * 4, axis=1)
    ids = ids + pltpu.roll(ids, 2 * SLOTS, 1)
    ids = ids + pltpu.roll(ids, SLOTS, 1)
    live = k < mine
    ids = jnp.where(live, ids, -1)
    pick = (iota((ATOMS_LOCAL, LANES), 0) == slots).astype(F32)
    copies[3].wait()
    pos = pos_ref[...]
    xyz = jnp.dot(pos, pick, precision=HIGHEST, preferred_element_type=F32)
    xyz_ref[...] = xyz
    part = lane // SLOTS
    row_out = jnp.where(part == 0, xyz[0:1], jnp.where(part == 1, xyz[1:2], xyz[2:3]))
    row_out = jnp.where(live, row_out, 0.0)
    row_out = jnp.where(part == 3, ids.astype(F32), row_out)
    out_ref[...] = jnp.broadcast_to(row_out, out_ref.shape)
    copies[4].wait()
    aux_ref[...] = jnp.concatenate([ids, slots, rank_ref[...]], axis=0)
    pair_forces(pos, pair_ref)


def dist_kernel(got_ref, frames_ref, out_ref, coded):
    got = got_ref[...]
    part = iota(got.shape, 1) // SLOTS
    ids = jnp.where(part == 3, got, 0.0)
    ids = ids + pltpu.roll(ids, 2 * SLOTS, 1)
    ids = ids + pltpu.roll(ids, SLOTS, 1)
    coded[0] = ids
    coded[1] = jnp.where(part == 3, 1.0, got)
    own = (holder_index() * BLOCK + iota((BLOCK, LANES), 0)).astype(F32)
    found = [jnp.zeros((BLOCK, LANES), F32) for _ in range(2)]
    for m in range(N_HOLDERS):
        hit = jnp.where(coded[0, m : m + 1, :] == own, coded[1, m : m + 1, :], 0.0)
        found[m % 2] = found[m % 2] + hit
    found = found[0] + found[1]
    part = iota((BLOCK, LANES), 1) // SLOTS
    column = [jnp.sum(jnp.where(part == c, found, 0.0), axis=1, keepdims=True) for c in range(4)]
    square = jnp.zeros((BLOCK, F), F32)
    for c in range(3):
        delta = column[c] - frames_ref[c * BLOCK : (c + 1) * BLOCK, :]
        square = square + delta * delta
    partial = jnp.sum(square * column[3], axis=0, keepdims=True) * (1.0 / P_SIZE)
    out_ref[...] = jnp.broadcast_to(partial, out_ref.shape)


def sum_kernel(got_ref, out_ref):
    out_ref[...] = jnp.broadcast_to(jnp.sum(got_ref[...], axis=0, keepdims=True), out_ref.shape)


def bias_kernel(got_ref, aux_ref, frames_ref, out_ref, cv_ref):
    dist = jnp.sum(got_ref[...], axis=0, keepdims=True)
    expo = -STRENGTH * dist
    top = jnp.max(expo, axis=1, keepdims=True)
    expd = jnp.exp(expo - top)
    total = jnp.sum(expd, axis=1, keepdims=True)
    weight = expd / total
    rank = aux_ref[2:3, :].astype(F32) / (F - 1.0)
    s_value = jnp.sum(rank * weight, axis=1, keepdims=True)
    z_value = -(top + jnp.log(total)) / STRENGTH
    grads = (
        KAPPA_S * P_SIZE * (s_value - S_HOME) * -STRENGTH * weight * (rank - s_value)
        + KAPPA_Z * P_SIZE * z_value * weight
    )
    lane = iota((1, LANES), 1)
    cv_ref[...] = jnp.where(lane == 0, s_value, z_value)
    eight = jnp.broadcast_to(grads, (8, F))
    dims = (((1,), (1,)), ((), ()))
    own = lax.dot_general(eight, frames_ref[...], dims, precision=HIGHEST, preferred_element_type=F32)
    whole = jnp.broadcast_to(jnp.sum(grads, axis=1, keepdims=True), (1, BLOCK))
    row = jnp.concatenate([own[0:1], whole], axis=1)
    out_ref[...] = jnp.broadcast_to(row, out_ref.shape)


def force_kernel(got_ref, aux_ref, xyz_ref, pair_ref, cv_in_ref, out_ref, cv_ref):
    cv_ref[...] = cv_in_ref[:, 0:2]
    ids = aux_ref[0:1, 0:SLOTS]
    slots = aux_ref[1:2, 0:SLOTS]
    from_row = (iota((N_HOLDERS, SLOTS), 0) == ids // BLOCK).astype(F32)
    dims = (((0,), (0,)), ((), ()))
    rows = lax.dot_general(got_ref[...], from_row, dims, precision=HIGHEST, preferred_element_type=F32)
    at = (iota((BLOCK, SLOTS), 0) == (ids & (BLOCK - 1))).astype(F32)
    whole = rows[96:97]
    bias = []
    for c in range(3):
        weighted = jnp.sum(rows[c * BLOCK : (c + 1) * BLOCK] * at, axis=0, keepdims=True)
        bias.append(xyz_ref[c : c + 1, 0:SLOTS] * whole - weighted)
    live = (ids >= 0).astype(F32)
    bias = jnp.concatenate(bias + bias[0:1] * 5, axis=0) * (live * (-2.0 / P_SIZE))
    pick = (iota((ATOMS_LOCAL, SLOTS), 0) == slots).astype(F32)
    dims = (((1,), (1,)), ((), ()))
    scattered = lax.dot_general(bias, pick, dims, precision=HIGHEST, preferred_element_type=F32)
    out_ref[...] = pair_ref[...] + scattered[0:3]


def spread(rows, axes):
    return lax.all_to_all(rows, axes, 0, 0, tiled=True)


def body(positions, frames, path_slot, path_count, path_order, frame_rank):
    frames = jnp.transpose(frames, (1, 2, 0)).reshape(3 * BLOCK, F)
    inputs = (
        path_count.reshape(4, LANES),
        path_order.reshape(32, LANES),
        path_slot,
        positions,
        frame_rank.reshape(1, F),
    )
    inputs = tuple(pltpu.with_memory_space_constraint(a, pltpu.HBM) for a in inputs)
    sent, aux, xyz, pair = call(
        pack_kernel,
        (
            shaped(N_HOLDERS, LANES),
            shaped(3, LANES, dtype=I32),
            shaped(3, LANES),
            shaped(3, ATOMS_LOCAL),
        ),
        "pack",
        inputs,
        in_specs=[HBM] * len(inputs),
        scratch_shapes=[pltpu.VMEM(a.shape, a.dtype) for a in inputs]
        + [pltpu.SemaphoreType.DMA((len(inputs),))],
        compiler_params=pltpu.CompilerParams(vmem_limit_bytes=8 << 20),
    )
    atoms = spread(sent, HOLDERS)
    coded = [pltpu.VMEM((2, N_HOLDERS, LANES), F32)]
    partial = small(dist_kernel, shaped(N_FIRST, LANES), "dist", (atoms, frames), coded)
    first = spread(partial, FIRST)
    row_sum = small(sum_kernel, shaped(N_SECOND, LANES), "sum", (first,))
    second = spread(row_sum, SECOND)
    biases, cv = small(
        bias_kernel, (shaped(N_HOLDERS, LANES), shaped(1, LANES)), "bias", (second, aux, frames)
    )
    back = spread(biases, HOLDERS)
    forces, cv = small(
        force_kernel, (shaped(3, ATOMS_LOCAL), shaped(1, 2)), "force", (back, aux, xyz, pair, cv)
    )
    return forces, cv.reshape(2)


def solution(mesh):
    finer = Mesh(mesh.devices.reshape(mesh.shape["gx"], mesh.shape["gy"], 8, 2), ALL)
    return jax.shard_map(
        body,
        mesh=finer,
        in_specs=(P(None, ALL), P(None, None, HOLDERS), P(ALL, None), P(), P(), P()),
        out_specs=(P(None, ALL), P()),
        check_vma=False,
    )
```

```python
import math

import jax
import jax.numpy as jnp
import numpy as np
from jax import lax
from jax.experimental import pallas as pl
from jax.experimental.pallas import tpu as pltpu
from jax.sharding import Mesh
from jax.sharding import PartitionSpec as P

P_SIZE = 4096
F = 128
ATOMS_LOCAL = 512
SLOTS = 32
LANES = 128
BLOCK = 32

ALL = ("gx", "gy", "gz_0", "gz_1")
HOLDERS = ("gy", "gz_0", "gz_1")
CHIPS = ("gy", "gz_0")
N_CHIPS = 64
IDS = 2 * BLOCK
FIRST = ("gz_0", "gz_1")
N_FIRST = 16
SECOND = ("gx", "gy")
N_SECOND = 32

LEAD = {"gx": 2, "gy": 5, "gz_0": 4, "gz_1": 1}
SIZE = {"gx": 4, "gy": 8, "gz_0": 8, "gz_1": 2}
TURN = LEAD["gy"] * 8 + LEAD["gz_0"]

STRENGTH = 20.0
S_HOME = 0.5
KAPPA_S = 0.5
KAPPA_Z = 0.05
PAIR_SCALE = 0.02
WIDTH_SQ = 4.0

HIGHEST = lax.Precision.HIGHEST
F32 = jnp.float32
I32 = jnp.int32
VMEM = pl.BlockSpec(memory_space=pltpu.VMEM)
HBM = pl.BlockSpec(memory_space=pltpu.HBM)


def holder_index():
    return lax.axis_index("gy") * 16 + lax.axis_index("gz_0") * 2 + lax.axis_index("gz_1")


def iota(shape, dim):
    return lax.broadcasted_iota(I32, shape, dim)


def shaped(*shape, dtype=F32):
    return jax.ShapeDtypeStruct(shape, dtype)


def call(kernel, out_shape, name, inputs, **kwargs):
    return pl.pallas_call(
        kernel,
        out_shape=out_shape,
        out_specs=jax.tree.map(lambda _: VMEM, out_shape),
        name=name,
        cost_estimate=pl.CostEstimate(flops=2000000, bytes_accessed=100000, transcendentals=0),
        **kwargs,
    )(*inputs)


def small(kernel, out_shape, name, inputs, scratch=()):
    return call(
        kernel,
        out_shape,
        name,
        inputs,
        in_specs=[VMEM] * len(inputs),
        scratch_shapes=scratch,
        compiler_params=pltpu.CompilerParams(vmem_limit_bytes=8 << 20),
    )


def pair_forces(pos, out_ref):
    columns = jnp.transpose(jnp.concatenate([pos, pos[0:1]] * 2, axis=0))
    scale = -1.0 / (WIDTH_SQ * math.log(2.0))
    step = 64
    sums = [jnp.zeros((8, ATOMS_LOCAL), F32) for _ in range(3)]
    for i in range(0, ATOMS_LOCAL, step):
        diff = [pos[c : c + 1, :] - columns[i : i + step, c : c + 1] for c in range(3)]
        dist_sq = diff[0] * diff[0] + diff[1] * diff[1] + diff[2] * diff[2]
        weight = jnp.exp2(dist_sq * scale)
        for c in range(3):
            term = weight * diff[c]
            for r in range(0, step, 8):
                sums[c] = sums[c] + term[r : r + 8]
    for c in range(3):
        out_ref[c : c + 1, :] = PAIR_SCALE * jnp.sum(sums[c], axis=0, keepdims=True)


def pack_kernel(
    count_hbm, order_hbm, slot_hbm, pos_hbm, rank_hbm, out_ref, aux_ref, xyz_ref, pair_ref, count_ref, order_ref, slot_ref, pos_ref, rank_ref, sems
):
    copies = [
        pltpu.make_async_copy(source, target, sems.at[i])
        for i, (source, target) in enumerate(
            (
                (count_hbm, count_ref),
                (order_hbm, order_ref),
                (slot_hbm, slot_ref),
                (pos_hbm, pos_ref),
                (rank_hbm, rank_ref),
            )
        )
    ]
    for copy in copies:
        copy.start()
    here = lax.axis_index("gx") * (2 * N_CHIPS) + holder_index()
    copies[0].wait()
    counts = count_ref[...]
    domain = iota(counts.shape, 0) * LANES + iota(counts.shape, 1)
    offset = jnp.sum(jnp.where(domain < here, counts, 0))
    mine = jnp.sum(jnp.where(domain == here, counts, 0))
    copies[1].wait()
    row = offset // LANES
    shift = offset - row * LANES
    first = order_ref[pl.ds(row, 1), :]
    second = order_ref[pl.ds(jnp.minimum(row + 1, P_SIZE // LANES - 1), 1), :]
    lane = iota((1, LANES), 1)
    k = lane & (SLOTS - 1)
    turn = jnp.where(shift == 0, 0, LANES - shift)
    ids = jnp.where(lane < LANES - shift, pltpu.roll(first, turn, 1), pltpu.roll(second, turn, 1))
    ids = jnp.where(lane < SLOTS, ids, 0)
    copies[2].wait()
    slots = jnp.concatenate([slot_ref[...]] * 4, axis=1)
    ids = ids + pltpu.roll(ids, 2 * SLOTS, 1)
    ids = ids + pltpu.roll(ids, SLOTS, 1)
    live = k < mine
    ids = jnp.where(live, ids, -1)
    pick = (iota((ATOMS_LOCAL, LANES), 0) == slots).astype(F32)
    copies[3].wait()
    pos = pos_ref[...]
    xyz = jnp.dot(pos, pick, precision=HIGHEST, preferred_element_type=F32)
    xyz_ref[...] = xyz
    part = lane // SLOTS
    row_out = jnp.where(part == 0, xyz[0:1], jnp.where(part == 1, xyz[1:2], xyz[2:3]))
    row_out = jnp.where(live, row_out, 0.0)
    row_out = jnp.where(part == 3, ids.astype(F32), row_out)
    out_ref[...] = jnp.broadcast_to(row_out, out_ref.shape)
    copies[4].wait()
    aux_ref[...] = jnp.concatenate([ids, slots, rank_ref[...]], axis=0)
    pair_forces(pos, pair_ref)


def dist_kernel(got_ref, mine_ref, other_ref, out_ref, coded):
    got = got_ref[...]
    part = iota(got.shape, 1) // SLOTS
    ids = jnp.where(part == 3, got, 0.0)
    ids = ids + pltpu.roll(ids, 2 * SLOTS, 1)
    ids = ids + pltpu.roll(ids, SLOTS, 1)
    coded[0] = ids
    coded[1] = jnp.where(part == 3, 1.0, got)
    j = iota((IDS, LANES), 0)
    own = ((holder_index() ^ (j // BLOCK)) * BLOCK + (j & (BLOCK - 1))).astype(F32)
    found = jnp.zeros((IDS, LANES), F32)
    for m in range(N_CHIPS):
        found = found + jnp.where(coded[0, m : m + 1, :] == own, coded[1, m : m + 1, :], 0.0)
    part = iota((IDS, LANES), 1) // SLOTS
    column = [jnp.sum(jnp.where(part == c, found, 0.0), axis=1, keepdims=True) for c in range(4)]
    total = jnp.zeros((BLOCK, F), F32)
    for half, frames_ref in enumerate((mine_ref, other_ref)):
        low = half * BLOCK
        square = jnp.zeros((BLOCK, F), F32)
        for c in range(3):
            delta = column[c][low : low + BLOCK] - frames_ref[c * BLOCK : (c + 1) * BLOCK, :]
            square = square + delta * delta
        total = total + square * column[3][low : low + BLOCK]
    partial = jnp.sum(total, axis=0, keepdims=True) * (1.0 / P_SIZE)
    out_ref[...] = jnp.broadcast_to(partial, out_ref.shape)


def sum_kernel(got_ref, out_ref):
    out_ref[...] = jnp.broadcast_to(jnp.sum(got_ref[...], axis=0, keepdims=True), out_ref.shape)


def bias_kernel(got_ref, aux_ref, mine_ref, other_ref, out_ref, cv_ref):
    dist = jnp.sum(got_ref[...], axis=0, keepdims=True)
    expo = -STRENGTH * dist
    top = jnp.max(expo, axis=1, keepdims=True)
    expd = jnp.exp(expo - top)
    total = jnp.sum(expd, axis=1, keepdims=True)
    weight = expd / total
    rank = aux_ref[2:3, :].astype(F32) / (F - 1.0)
    s_value = jnp.sum(rank * weight, axis=1, keepdims=True)
    z_value = -(top + jnp.log(total)) / STRENGTH
    grads = (
        KAPPA_S * P_SIZE * (s_value - S_HOME) * -STRENGTH * weight * (rank - s_value)
        + KAPPA_Z * P_SIZE * z_value * weight
    )
    lane = iota((1, LANES), 1)
    cv_ref[...] = jnp.where(lane == 0, s_value, z_value)
    eight = jnp.broadcast_to(grads, (8, F))
    dims = (((1,), (1,)), ((), ()))
    whole = jnp.broadcast_to(jnp.sum(grads, axis=1, keepdims=True), (1, BLOCK))
    rows = []
    for frames_ref in (mine_ref, other_ref):
        sums = lax.dot_general(
            eight, frames_ref[...], dims, precision=HIGHEST, preferred_element_type=F32
        )
        rows.append(jnp.concatenate([sums[0:1], whole], axis=1))
    out_ref[...] = jnp.where((iota(out_ref.shape, 0) & 1) == 0, rows[0], rows[1])


def force_kernel(got_ref, aux_ref, xyz_ref, pair_ref, cv_in_ref, out_ref, cv_ref):
    cv_ref[...] = cv_in_ref[:, 0:2]
    ids = aux_ref[0:1, 0:SLOTS]
    slots = aux_ref[1:2, 0:SLOTS]
    source = (ids // BLOCK) ^ (2 * TURN) ^ lax.axis_index("gz_1")
    from_row = (iota((2 * N_CHIPS, SLOTS), 0) == source).astype(F32)
    dims = (((0,), (0,)), ((), ()))
    rows = lax.dot_general(got_ref[...], from_row, dims, precision=HIGHEST, preferred_element_type=F32)
    at = (iota((BLOCK, SLOTS), 0) == (ids & (BLOCK - 1))).astype(F32)
    whole = rows[96:97]
    bias = []
    for c in range(3):
        weighted = jnp.sum(rows[c * BLOCK : (c + 1) * BLOCK] * at, axis=0, keepdims=True)
        bias.append(xyz_ref[c : c + 1, 0:SLOTS] * whole - weighted)
    live = (ids >= 0).astype(F32)
    bias = jnp.concatenate(bias + bias[0:1] * 5, axis=0) * (live * (-2.0 / P_SIZE))
    pick = (iota((ATOMS_LOCAL, SLOTS), 0) == slots).astype(F32)
    dims = (((1,), (1,)), ((), ()))
    scattered = lax.dot_general(bias, pick, dims, precision=HIGHEST, preferred_element_type=F32)
    out_ref[...] = pair_ref[...] + scattered[0:3]


def groups_of(axes):
    index = np.arange(math.prod(SIZE.values())).reshape(tuple(SIZE.values()))
    rest = [n for n, axis in enumerate(ALL) if axis not in axes]
    for axis in axes:
        index = np.take(index, np.arange(SIZE[axis]) ^ LEAD[axis], axis=ALL.index(axis))
    index = np.transpose(index, rest + [ALL.index(axis) for axis in axes])
    return index.reshape(-1, math.prod(SIZE[axis] for axis in axes)).tolist()


def spread(rows, axes):
    return lax.all_to_all(rows, ALL, 0, 0, tiled=True, axis_index_groups=groups_of(axes))


def body(positions, frames, path_slot, path_count, path_order, frame_rank):
    mine = jnp.transpose(frames, (1, 2, 0)).reshape(3 * BLOCK, F)
    other = lax.ppermute(mine, "gz_1", [(0, 1), (1, 0)])
    inputs = (
        path_count.reshape(4, LANES),
        path_order.reshape(32, LANES),
        path_slot,
        positions,
        frame_rank.reshape(1, F),
    )
    inputs = tuple(pltpu.with_memory_space_constraint(a, pltpu.HBM) for a in inputs)
    sent, aux, xyz, pair = call(
        pack_kernel,
        (
            shaped(N_CHIPS, LANES),
            shaped(3, LANES, dtype=I32),
            shaped(3, LANES),
            shaped(3, ATOMS_LOCAL),
        ),
        "pack",
        inputs,
        in_specs=[HBM] * len(inputs),
        scratch_shapes=[pltpu.VMEM(a.shape, a.dtype) for a in inputs]
        + [pltpu.SemaphoreType.DMA((len(inputs),))],
        compiler_params=pltpu.CompilerParams(vmem_limit_bytes=8 << 20),
    )
    atoms = spread(sent, CHIPS)
    coded = [pltpu.VMEM((2, N_CHIPS, LANES), F32)]
    partial = small(dist_kernel, shaped(N_FIRST, LANES), "dist", (atoms, mine, other), coded)
    first = spread(partial, FIRST)
    row_sum = small(sum_kernel, shaped(N_SECOND, LANES), "sum", (first,))
    second = spread(row_sum, SECOND)
    biases, cv = small(
        bias_kernel,
        (shaped(2 * N_CHIPS, LANES), shaped(1, LANES)),
        "bias",
        (second, aux, mine, other),
    )
    back = spread(biases, CHIPS)
    forces, cv = small(
        force_kernel, (shaped(3, ATOMS_LOCAL), shaped(1, 2)), "force", (back, aux, xyz, pair, cv)
    )
    return forces, cv.reshape(2)


def solution(mesh):
    finer = Mesh(mesh.devices.reshape(mesh.shape["gx"], mesh.shape["gy"], 8, 2), ALL)
    return jax.shard_map(
        body,
        mesh=finer,
        in_specs=(P(None, ALL), P(None, None, HOLDERS), P(ALL, None), P(), P(), P()),
        out_specs=(P(None, ALL), P()),
        check_vma=False,
    )
```

```python
import math

import jax
import jax.numpy as jnp
from jax import lax
from jax.experimental import pallas as pl
from jax.experimental.pallas import tpu as pltpu
from jax.sharding import Mesh
from jax.sharding import PartitionSpec as P


P_SIZE = 4096
F = 128
ATOMS_LOCAL = 512
SLOTS = 32
LANES = 128
BLOCK = 32

ALL = ("gx", "gy", "gz_0", "gz_1")
HOLDERS = ("gy", "gz_0", "gz_1")
N_CHIPS = 64
IDS = 2 * BLOCK
N_FIRST = 16
N_SECOND = 32

X_FIRST, Y_FIRST = 2, 4
Z_FIRST = (5, 5)
TURN = tuple(16 * z + 2 * Y_FIRST for z in Z_FIRST)


def middle(z):
    return ((z + 2) & 4) // 4


STRENGTH = 20.0
S_HOME = 0.5
KAPPA_S = 0.5
KAPPA_Z = 0.05
PAIR_SCALE = 0.02
WIDTH_SQ = 4.0

HIGHEST = lax.Precision.HIGHEST
F32 = jnp.float32
I32 = jnp.int32
VMEM = pl.BlockSpec(memory_space=pltpu.VMEM)
HBM = pl.BlockSpec(memory_space=pltpu.HBM)


def holder_index():
    return lax.axis_index("gy") * 16 + lax.axis_index("gz_0") * 2 + lax.axis_index("gz_1")


def iota(shape, dim):
    return lax.broadcasted_iota(I32, shape, dim)


def shaped(*shape, dtype=F32):
    return jax.ShapeDtypeStruct(shape, dtype)


def call(kernel, out_shape, inputs, **kwargs):
    return pl.pallas_call(
        kernel,
        out_shape=out_shape,
        out_specs=jax.tree.map(lambda _: VMEM, out_shape),
        cost_estimate=pl.CostEstimate(flops=2000000, bytes_accessed=100000, transcendentals=0),
        **kwargs,
    )(*inputs)


def small(kernel, out_shape, inputs, scratch=()):
    return call(
        kernel,
        out_shape,
        inputs,
        in_specs=[VMEM] * len(inputs),
        scratch_shapes=scratch,
        compiler_params=pltpu.CompilerParams(vmem_limit_bytes=8 << 20),
    )


def pair_kernel(pos_ref, out_ref):
    pos = pos_ref[...]
    columns = jnp.transpose(jnp.concatenate([pos, pos[0:1]] * 2, axis=0))
    scale = -1.0 / (WIDTH_SQ * math.log(2.0))
    step = 64
    sums = [jnp.zeros((8, ATOMS_LOCAL), F32) for _ in range(3)]
    for i in range(0, ATOMS_LOCAL, step):
        diff = [pos[c : c + 1, :] - columns[i : i + step, c : c + 1] for c in range(3)]
        dist_sq = diff[0] * diff[0] + diff[1] * diff[1] + diff[2] * diff[2]
        weight = jnp.exp2(dist_sq * scale)
        for c in range(3):
            term = weight * diff[c]
            for r in range(0, step, 8):
                sums[c] = sums[c] + term[r : r + 8]
    for c in range(3):
        out_ref[c : c + 1, :] = PAIR_SCALE * jnp.sum(sums[c], axis=0, keepdims=True)


def pack_kernel(
    count_hbm, order_hbm, slot_hbm, pos_hbm, rank_hbm, out_ref, aux_ref, xyz_ref, pos_out_ref, count_ref, order_ref, slot_ref, pos_ref, rank_ref, sems
):
    copies = [
        pltpu.make_async_copy(source, target, sems.at[i])
        for i, (source, target) in enumerate(
            (
                (count_hbm, count_ref),
                (order_hbm, order_ref),
                (slot_hbm, slot_ref),
                (pos_hbm, pos_ref),
                (rank_hbm, rank_ref),
            )
        )
    ]
    for copy in copies:
        copy.start()
    here = lax.axis_index("gx") * (2 * N_CHIPS) + holder_index()
    for copy in copies:
        copy.wait()
    counts = count_ref[...]
    domain = iota(counts.shape, 0) * LANES + iota(counts.shape, 1)
    offset = jnp.sum(jnp.where(domain < here, counts, 0))
    mine = jnp.where(domain == here, counts, 0)
    mine = jnp.sum(jnp.sum(mine, axis=0, keepdims=True), axis=1, keepdims=True)
    slots = jnp.concatenate([slot_ref[...]] * 4, axis=1)
    pick = (iota((ATOMS_LOCAL, LANES), 0) == slots).astype(F32)
    pos = pos_ref[...]
    xyz = jnp.dot(pos, pick, precision=HIGHEST, preferred_element_type=F32)
    lane = iota((1, LANES), 1)
    k = lane & (SLOTS - 1)
    live = k < mine
    row = offset // LANES
    shift = offset - row * LANES
    first = order_ref[pl.ds(row, 1), :]
    second = order_ref[pl.ds(jnp.minimum(row + 1, P_SIZE // LANES - 1), 1), :]
    ids = jnp.full((1, LANES), -1, I32)
    for part in range(4):
        start = shift - part * SLOTS
        turn = jnp.where(start <= 0, -start, LANES - start)
        here_first = k < LANES - shift
        turned = jnp.where(here_first, pltpu.roll(first, turn, 1), pltpu.roll(second, turn, 1))
        ids = jnp.where(live & (lane // SLOTS == part), turned, ids)
    xyz_ref[...] = xyz
    part = lane // SLOTS
    row_out = jnp.where(part == 0, xyz[0:1], jnp.where(part == 1, xyz[1:2], xyz[2:3]))
    row_out = jnp.where(live, row_out, 0.0)
    row_out = jnp.where(part == 3, ids.astype(F32), row_out)
    out_ref[...] = jnp.broadcast_to(row_out, out_ref.shape)
    aux_ref[...] = jnp.concatenate([ids, slots, rank_ref[...]], axis=0)
    pos_out_ref[...] = pos


def dist_kernel(got_ref, mine_ref, other_ref, out_ref, coded):
    got = got_ref[...]
    part = iota(got.shape, 1) // SLOTS
    ids = jnp.where(part == 3, got, 0.0)
    ids = ids + pltpu.roll(ids, 2 * SLOTS, 1)
    ids = ids + pltpu.roll(ids, SLOTS, 1)
    coded[0] = ids
    coded[1] = jnp.where(part == 3, 1.0, got)
    j = iota((IDS, LANES), 0)
    own = ((holder_index() ^ (j // BLOCK)) * BLOCK + (j & (BLOCK - 1))).astype(F32)
    found = jnp.zeros((IDS, LANES), F32)
    for m in range(N_CHIPS):
        found = found + jnp.where(coded[0, m : m + 1, :] == own, coded[1, m : m + 1, :], 0.0)
    part = iota((IDS, LANES), 1) // SLOTS
    column = [jnp.sum(jnp.where(part == c, found, 0.0), axis=1, keepdims=True) for c in range(4)]
    total = jnp.zeros((BLOCK, F), F32)
    for half, frames_ref in enumerate((mine_ref, other_ref)):
        low = half * BLOCK
        square = jnp.zeros((BLOCK, F), F32)
        for c in range(3):
            delta = column[c][low : low + BLOCK] - frames_ref[c * BLOCK : (c + 1) * BLOCK, :]
            square = square + delta * delta
        total = total + square * column[3][low : low + BLOCK]
    partial = jnp.sum(total, axis=0, keepdims=True) * (1.0 / P_SIZE)
    out_ref[...] = jnp.broadcast_to(partial, out_ref.shape)


def sum_kernel(got_ref, out_ref):
    out_ref[...] = jnp.broadcast_to(jnp.sum(got_ref[...], axis=0, keepdims=True), out_ref.shape)


def bias_kernel(got_ref, aux_ref, mine_ref, other_ref, out_ref, cv_ref):
    dist = jnp.sum(got_ref[...], axis=0, keepdims=True)
    expo = -STRENGTH * dist
    top = jnp.max(expo, axis=1, keepdims=True)
    expd = jnp.exp(expo - top)
    rank = aux_ref[2:3, :].astype(F32) / (F - 1.0)
    total = jnp.sum(expd, axis=1, keepdims=True)
    ranked = jnp.sum(rank * expd, axis=1, keepdims=True)
    s_value = ranked / total
    z_value = -(top + jnp.log(total)) / STRENGTH
    weight = expd / total
    grads = (
        KAPPA_S * P_SIZE * (s_value - S_HOME) * -STRENGTH * weight * (rank - s_value)
        + KAPPA_Z * P_SIZE * z_value * weight
    )
    lane = iota((1, LANES), 1)
    cv_ref[...] = jnp.where(lane == 0, s_value, z_value)
    eight = jnp.broadcast_to(grads, (8, F))
    dims = (((1,), (1,)), ((), ()))
    ones = jnp.ones((BLOCK, F), F32)
    rows = []
    for frames_ref in (mine_ref, other_ref):
        against = jnp.concatenate([frames_ref[...], ones], axis=0)
        sums = lax.dot_general(eight, against, dims, precision=HIGHEST, preferred_element_type=F32)
        rows.append(sums[0:1])
    out_ref[...] = jnp.where((iota(out_ref.shape, 0) & 1) == 0, rows[0], rows[1])


def force_kernel(got_ref, aux_ref, xyz_ref, pair_ref, cv_in_ref, out_ref, cv_ref):
    cv_ref[...] = cv_in_ref[:, 0:2]
    ids = aux_ref[0:1, 0:SLOTS]
    slots = aux_ref[1:2, 0:SLOTS]
    half = lax.axis_index("gz_1") ^ middle(lax.axis_index("gy"))
    turn = TURN[0] + half * (TURN[1] - TURN[0])
    source = (ids // BLOCK) ^ turn ^ half ^ middle(ids // (16 * BLOCK))
    from_row = (iota((2 * N_CHIPS, SLOTS), 0) == source).astype(F32)
    dims = (((0,), (0,)), ((), ()))
    rows = lax.dot_general(got_ref[...], from_row, dims, precision=HIGHEST, preferred_element_type=F32)
    at = (iota((BLOCK, SLOTS), 0) == (ids & (BLOCK - 1))).astype(F32)
    whole = rows[96:97]
    bias = []
    for c in range(3):
        weighted = jnp.sum(rows[c * BLOCK : (c + 1) * BLOCK] * at, axis=0, keepdims=True)
        bias.append(xyz_ref[c : c + 1, 0:SLOTS] * whole - weighted)
    live = (ids >= 0).astype(F32)
    bias = jnp.concatenate(bias + bias[0:1] * 5, axis=0) * (live * (-2.0 / P_SIZE))
    pick = (iota((ATOMS_LOCAL, SLOTS), 0) == slots).astype(F32)
    dims = (((1,), (1,)), ((), ()))
    scattered = lax.dot_general(bias, pick, dims, precision=HIGHEST, preferred_element_type=F32)
    out_ref[...] = pair_ref[...] + scattered[0:3]


def device(x, z, y, core):
    return ((x * 8 + z) * 8 + y) * 2 + core


def chip_groups():
    return [
        [
            device(x, z ^ Z_FIRST[half], y ^ Y_FIRST, half ^ middle(z ^ Z_FIRST[half]))
            for z in range(8)
            for y in range(8)
        ]
        for x in range(4)
        for half in range(2)
    ]


def first_groups():
    return [
        [device(x, z, y ^ Y_FIRST, core ^ 1) for y in range(8) for core in range(2)]
        for x in range(4)
        for z in range(8)
    ]


def second_groups():
    return [
        [
            device(x ^ X_FIRST, z ^ Z_FIRST[half], y, half ^ middle(z ^ Z_FIRST[half]))
            for x in range(4)
            for z in range(8)
        ]
        for y in range(8)
        for half in range(2)
    ]


def spread(rows, groups):
    return lax.all_to_all(rows, ALL, 0, 0, tiled=True, axis_index_groups=groups)


def body(positions, frames, path_slot, path_count, path_order, frame_rank):
    mine = jnp.transpose(frames, (1, 2, 0)).reshape(3 * BLOCK, F)
    other = lax.ppermute(mine, "gz_1", [(0, 1), (1, 0)])
    inputs = (
        path_count.reshape(4, LANES),
        path_order.reshape(32, LANES),
        path_slot,
        positions,
        frame_rank.reshape(1, F),
    )
    inputs = tuple(pltpu.with_memory_space_constraint(a, pltpu.HBM) for a in inputs)
    sent, aux, xyz, pos = call(
        pack_kernel,
        (
            shaped(N_CHIPS, LANES),
            shaped(3, LANES, dtype=I32),
            shaped(3, LANES),
            shaped(3, ATOMS_LOCAL),
        ),
        inputs,
        in_specs=[HBM] * len(inputs),
        scratch_shapes=[pltpu.VMEM(a.shape, a.dtype) for a in inputs]
        + [pltpu.SemaphoreType.DMA((len(inputs),))],
        compiler_params=pltpu.CompilerParams(vmem_limit_bytes=8 << 20),
    )
    atoms = spread(sent, chip_groups())
    coded = [pltpu.VMEM((2, N_CHIPS, LANES), F32)]
    partial = small(dist_kernel, shaped(N_FIRST, LANES), (atoms, mine, other), coded)
    first = spread(partial, first_groups())
    row_sum = small(sum_kernel, shaped(N_SECOND, LANES), (first,))
    second = spread(row_sum, second_groups())
    biases, cv = small(
        bias_kernel, (shaped(2 * N_CHIPS, LANES), shaped(1, LANES)), (second, aux, mine, other)
    )
    back = spread(biases, chip_groups())
    pair = small(pair_kernel, shaped(3, ATOMS_LOCAL), (pos,))
    forces, cv = small(
        force_kernel, (shaped(3, ATOMS_LOCAL), shaped(1, 2)), (back, aux, xyz, pair, cv)
    )
    return forces, cv.reshape(2)


def solution(mesh):
    finer = Mesh(mesh.devices.reshape(mesh.shape["gx"], mesh.shape["gy"], 8, 2), ALL)
    return jax.shard_map(
        body,
        mesh=finer,
        in_specs=(P(None, ALL), P(None, None, HOLDERS), P(ALL, None), P(), P(), P()),
        out_specs=(P(None, ALL), P()),
        check_vma=False,
    )
```

```python
import math

import jax
import jax.numpy as jnp
from jax import lax
from jax.experimental import pallas as pl
from jax.experimental.pallas import tpu as pltpu
from jax.sharding import Mesh
from jax.sharding import PartitionSpec as P


P_SIZE = 4096
F = 128
ATOMS_LOCAL = 512
SLOTS = 32
LANES = 128
BLOCK = 32

ALL = ("gx", "gy", "gz_0", "gz_1")
HOLDERS = ("gy", "gz_0", "gz_1")
N_CHIPS = 64
IDS = 2 * BLOCK
N_FIRST = 16
N_SECOND = 32

ATOMS_FIRST = (5, 5)
FIRST_FIRST = 4
SECOND_FIRST = (2, 5)
BIAS_FIRST = (4, 4)
TURN = 16 * BIAS_FIRST[0] + 2 * BIAS_FIRST[1]


def middle(z):
    return ((z + 2) & 4) // 4


STRENGTH = 20.0
S_HOME = 0.5
KAPPA_S = 0.5
KAPPA_Z = 0.05
PAIR_SCALE = 0.02
WIDTH_SQ = 4.0

HIGHEST = lax.Precision.HIGHEST
F32 = jnp.float32
I32 = jnp.int32
VMEM = pl.BlockSpec(memory_space=pltpu.VMEM)
HBM = pl.BlockSpec(memory_space=pltpu.HBM)


def holder_index():
    return lax.axis_index("gy") * 16 + lax.axis_index("gz_0") * 2 + lax.axis_index("gz_1")


def iota(shape, dim):
    return lax.broadcasted_iota(I32, shape, dim)


def shaped(*shape, dtype=F32):
    return jax.ShapeDtypeStruct(shape, dtype)


def call(kernel, out_shape, inputs, **kwargs):
    return pl.pallas_call(
        kernel,
        out_shape=out_shape,
        out_specs=jax.tree.map(lambda _: VMEM, out_shape),
        cost_estimate=pl.CostEstimate(flops=2000000, bytes_accessed=100000, transcendentals=0),
        **kwargs,
    )(*inputs)


def small(kernel, out_shape, inputs, scratch=()):
    return call(
        kernel,
        out_shape,
        inputs,
        in_specs=[VMEM] * len(inputs),
        scratch_shapes=scratch,
        compiler_params=pltpu.CompilerParams(vmem_limit_bytes=8 << 20),
    )


def pair_kernel(pos_ref, aux_ref, xyz_ref, out_ref, select_ref, part_ref, pick_ref):
    columns = [aux_ref[0:2, :].astype(F32), xyz_ref[...], xyz_ref[...]]
    columns = jnp.transpose(jnp.concatenate(columns, axis=0))[0:SLOTS]
    ids = columns[:, 0:1].astype(I32)
    slots = columns[:, 1:2].astype(I32)
    half = lax.axis_index("gz_1") ^ middle(lax.axis_index("gy"))
    source = (ids // BLOCK) ^ TURN ^ half ^ middle(ids // (16 * BLOCK))
    lane = iota((SLOTS, LANES), 1)
    select_ref[...] = (lane == source).astype(F32)
    scale = jnp.where(ids >= 0, -2.0 / P_SIZE, 0.0)
    for c in range(3):
        at = (lane == c * BLOCK + (ids & (BLOCK - 1))).astype(F32)
        whole = jnp.where(lane == 3 * BLOCK, columns[:, c + 2 : c + 3], 0.0)
        part_ref[c * SLOTS : (c + 1) * SLOTS, :] = scale * (whole - at)
    pick_ref[...] = (iota((SLOTS, ATOMS_LOCAL), 1) == slots).astype(F32)
    pos = pos_ref[...]
    columns = jnp.transpose(jnp.concatenate([pos, pos[0:1]] * 2, axis=0))
    scale = -1.0 / (WIDTH_SQ * math.log(2.0))
    step = 64
    sums = [jnp.zeros((8, ATOMS_LOCAL), F32) for _ in range(3)]
    for i in range(0, ATOMS_LOCAL, step):
        diff = [pos[c : c + 1, :] - columns[i : i + step, c : c + 1] for c in range(3)]
        dist_sq = diff[0] * diff[0] + diff[1] * diff[1] + diff[2] * diff[2]
        weight = jnp.exp2(dist_sq * scale)
        for c in range(3):
            term = weight * diff[c]
            for r in range(0, step, 8):
                sums[c] = sums[c] + term[r : r + 8]
    for c in range(3):
        out_ref[c : c + 1, :] = PAIR_SCALE * jnp.sum(sums[c], axis=0, keepdims=True)


def pack_kernel(
    count_hbm, order_hbm, slot_hbm, pos_hbm, rank_hbm, out_ref, aux_ref, xyz_ref, pos_out_ref, count_ref, order_ref, slot_ref, pos_ref, rank_ref, sems
):
    copies = [
        pltpu.make_async_copy(source, target, sems.at[i])
        for i, (source, target) in enumerate(
            (
                (count_hbm, count_ref),
                (order_hbm, order_ref),
                (slot_hbm, slot_ref),
                (pos_hbm, pos_ref),
                (rank_hbm, rank_ref),
            )
        )
    ]
    for copy in copies:
        copy.start()
    here = lax.axis_index("gx") * (2 * N_CHIPS) + holder_index()
    for copy in copies:
        copy.wait()
    counts = count_ref[...]
    domain = iota(counts.shape, 0) * LANES + iota(counts.shape, 1)
    offset = jnp.sum(jnp.where(domain < here, counts, 0))
    mine = jnp.where(domain == here, counts, 0)
    mine = jnp.sum(jnp.sum(mine, axis=0, keepdims=True), axis=1, keepdims=True)
    slots = jnp.concatenate([slot_ref[...]] * 4, axis=1)
    pick = (iota((ATOMS_LOCAL, LANES), 0) == slots).astype(F32)
    pos = pos_ref[...]
    xyz = jnp.dot(pos, pick, precision=HIGHEST, preferred_element_type=F32)
    lane = iota((1, LANES), 1)
    k = lane & (SLOTS - 1)
    live = k < mine
    row = offset // LANES
    shift = offset - row * LANES
    first = order_ref[pl.ds(row, 1), :]
    second = order_ref[pl.ds(jnp.minimum(row + 1, P_SIZE // LANES - 1), 1), :]
    ids = jnp.full((1, LANES), -1, I32)
    for part in range(4):
        start = shift - part * SLOTS
        turn = jnp.where(start <= 0, -start, LANES - start)
        here_first = k < LANES - shift
        turned = jnp.where(here_first, pltpu.roll(first, turn, 1), pltpu.roll(second, turn, 1))
        ids = jnp.where(live & (lane // SLOTS == part), turned, ids)
    xyz_ref[...] = xyz
    part = lane // SLOTS
    row_out = jnp.where(part == 0, xyz[0:1], jnp.where(part == 1, xyz[1:2], xyz[2:3]))
    row_out = jnp.where(live, row_out, 0.0)
    row_out = jnp.where(part == 3, ids.astype(F32), row_out)
    out_ref[...] = jnp.broadcast_to(row_out, out_ref.shape)
    aux_ref[...] = jnp.concatenate([ids, slots, rank_ref[...]], axis=0)
    pos_out_ref[...] = pos


def dist_kernel(got_ref, mine_ref, other_ref, out_ref, coded):
    got = got_ref[...]
    part = iota(got.shape, 1) // SLOTS
    ids = jnp.where(part == 3, got, 0.0)
    ids = ids + pltpu.roll(ids, 2 * SLOTS, 1)
    ids = ids + pltpu.roll(ids, SLOTS, 1)
    coded[0] = ids
    coded[1] = jnp.where(part == 3, 1.0, got)
    j = iota((IDS, LANES), 0)
    own = ((holder_index() ^ (j // BLOCK)) * BLOCK + (j & (BLOCK - 1))).astype(F32)
    found = jnp.zeros((IDS, LANES), F32)
    for m in range(N_CHIPS):
        found = found + jnp.where(coded[0, m : m + 1, :] == own, coded[1, m : m + 1, :], 0.0)
    part = iota((IDS, LANES), 1) // SLOTS
    column = [jnp.sum(jnp.where(part == c, found, 0.0), axis=1, keepdims=True) for c in range(4)]
    total = jnp.zeros((BLOCK, F), F32)
    for half, frames_ref in enumerate((mine_ref, other_ref)):
        low = half * BLOCK
        square = jnp.zeros((BLOCK, F), F32)
        for c in range(3):
            delta = column[c][low : low + BLOCK] - frames_ref[c * BLOCK : (c + 1) * BLOCK, :]
            square = square + delta * delta
        total = total + square * column[3][low : low + BLOCK]
    partial = jnp.sum(total, axis=0, keepdims=True) * (1.0 / P_SIZE)
    out_ref[...] = jnp.broadcast_to(partial, out_ref.shape)


def sum_kernel(got_ref, out_ref):
    out_ref[...] = jnp.broadcast_to(jnp.sum(got_ref[...], axis=0, keepdims=True), out_ref.shape)


def bias_kernel(got_ref, aux_ref, mine_ref, other_ref, out_ref, cv_ref):
    dist = jnp.sum(got_ref[...], axis=0, keepdims=True)
    expo = -STRENGTH * dist
    top = jnp.max(expo, axis=1, keepdims=True)
    expd = jnp.exp(expo - top)
    rank = aux_ref[2:3, :].astype(F32) / (F - 1.0)
    total = jnp.sum(expd, axis=1, keepdims=True)
    ranked = jnp.sum(rank * expd, axis=1, keepdims=True)
    s_value = ranked / total
    z_value = -(top + jnp.log(total)) / STRENGTH
    weight = expd / total
    grads = (
        KAPPA_S * P_SIZE * (s_value - S_HOME) * -STRENGTH * weight * (rank - s_value)
        + KAPPA_Z * P_SIZE * z_value * weight
    )
    lane = iota((1, LANES), 1)
    cv_ref[...] = jnp.where(lane == 0, s_value, z_value)
    eight = jnp.broadcast_to(grads, (8, F))
    dims = (((1,), (1,)), ((), ()))
    ones = jnp.ones((BLOCK, F), F32)
    rows = []
    for frames_ref in (mine_ref, other_ref):
        against = jnp.concatenate([frames_ref[...], ones], axis=0)
        sums = lax.dot_general(eight, against, dims, precision=HIGHEST, preferred_element_type=F32)
        rows.append(sums[0:1])
    out_ref[...] = jnp.where((iota(out_ref.shape, 0) & 1) == 0, rows[0], rows[1])


def force_kernel(got_ref, select_ref, part_ref, pick_ref, pair_ref, cv_in_ref, out_ref, cv_ref):
    cv_ref[...] = cv_in_ref[:, 0:2]
    got = got_ref[...]
    high = got.astype(jnp.bfloat16)
    rest = got - high.astype(F32)
    mid = rest.astype(jnp.bfloat16)
    low = (rest - mid.astype(F32)).astype(jnp.bfloat16)
    select = select_ref[...].astype(jnp.bfloat16)
    rows = [jnp.dot(select, piece, preferred_element_type=F32) for piece in (low, mid, high)]
    rows = (rows[0] + rows[1]) + rows[2]
    pick = pick_ref[...]
    for c in range(3):
        part = part_ref[c * SLOTS : (c + 1) * SLOTS, :]
        bias = jnp.sum(rows * part, axis=1, keepdims=True)
        total = jnp.sum(bias * pick, axis=0, keepdims=True)
        out_ref[c : c + 1, :] = pair_ref[c : c + 1, :] + total


def device(x, z, y, core):
    return ((x * 8 + z) * 8 + y) * 2 + core


def chip_groups(first):
    return [
        [
            device(x, z ^ first[0], y ^ first[1], half ^ middle(z ^ first[0]))
            for z in range(8)
            for y in range(8)
        ]
        for x in range(4)
        for half in range(2)
    ]


def first_groups():
    return [
        [device(x, z, y ^ FIRST_FIRST, core ^ 1) for y in range(8) for core in range(2)]
        for x in range(4)
        for z in range(8)
    ]


def second_groups():
    first = SECOND_FIRST
    return [
        [
            device(x ^ first[0], z ^ first[1], y, half ^ middle(z ^ first[1]))
            for x in range(4)
            for z in range(8)
        ]
        for y in range(8)
        for half in range(2)
    ]


def spread(rows, groups):
    return lax.all_to_all(rows, ALL, 0, 0, tiled=True, axis_index_groups=groups)


def body(positions, frames, path_slot, path_count, path_order, frame_rank):
    mine = jnp.transpose(frames, (1, 2, 0)).reshape(3 * BLOCK, F)
    other = lax.ppermute(mine, "gz_1", [(0, 1), (1, 0)])
    inputs = (
        path_count.reshape(4, LANES),
        path_order.reshape(32, LANES),
        path_slot,
        positions,
        frame_rank.reshape(1, F),
    )
    inputs = tuple(pltpu.with_memory_space_constraint(a, pltpu.HBM) for a in inputs)
    sent, aux, xyz, pos = call(
        pack_kernel,
        (
            shaped(N_CHIPS, LANES),
            shaped(3, LANES, dtype=I32),
            shaped(3, LANES),
            shaped(3, ATOMS_LOCAL),
        ),
        inputs,
        in_specs=[HBM] * len(inputs),
        scratch_shapes=[pltpu.VMEM(a.shape, a.dtype) for a in inputs]
        + [pltpu.SemaphoreType.DMA((len(inputs),))],
        compiler_params=pltpu.CompilerParams(vmem_limit_bytes=8 << 20),
    )
    atoms = spread(sent, chip_groups(ATOMS_FIRST))
    coded = [pltpu.VMEM((2, N_CHIPS, LANES), F32)]
    partial = small(dist_kernel, shaped(N_FIRST, LANES), (atoms, mine, other), coded)
    first = spread(partial, first_groups())
    row_sum = small(sum_kernel, shaped(N_SECOND, LANES), (first,))
    second = spread(row_sum, second_groups())
    biases, cv = small(
        bias_kernel, (shaped(2 * N_CHIPS, LANES), shaped(1, LANES)), (second, aux, mine, other)
    )
    back = spread(biases, chip_groups(BIAS_FIRST))
    pair, select, part, pick = small(
        pair_kernel,
        (
            shaped(3, ATOMS_LOCAL),
            shaped(SLOTS, LANES),
            shaped(3 * SLOTS, LANES),
            shaped(SLOTS, ATOMS_LOCAL),
        ),
        (pos, aux, xyz),
    )
    forces, cv = small(
        force_kernel, (shaped(3, ATOMS_LOCAL), shaped(1, 2)), (back, select, part, pick, pair, cv)
    )
    return forces, cv.reshape(2)


def solution(mesh):
    finer = Mesh(mesh.devices.reshape(mesh.shape["gx"], mesh.shape["gy"], 8, 2), ALL)
    return jax.shard_map(
        body,
        mesh=finer,
        in_specs=(P(None, ALL), P(None, None, HOLDERS), P(ALL, None), P(), P(), P()),
        out_specs=(P(None, ALL), P()),
        check_vma=False,
    )
```

```python
import math

import jax
import jax.numpy as jnp
from jax import lax
from jax.experimental import pallas as pl
from jax.experimental.pallas import tpu as pltpu
from jax.sharding import Mesh
from jax.sharding import PartitionSpec as P


P_SIZE = 4096
F = 128
ATOMS_LOCAL = 512
SLOTS = 32
LANES = 128
BLOCK = 32

ALL = ("gx", "gy", "gz_0", "gz_1")
HOLDERS = ("gy", "gz_0", "gz_1")
N_CHIPS = 64
IDS = 2 * BLOCK
N_FIRST = 16
N_SECOND = 32

ATOMS_FIRST = (5, 5)
FIRST_FIRST = 4
SECOND_FIRST = (2, 5)
BIAS_FIRST = (4, 4)
TURN = 16 * BIAS_FIRST[0] + 2 * BIAS_FIRST[1]


def middle(z):
    return ((z + 2) & 4) // 4


STRENGTH = 20.0
S_HOME = 0.5
KAPPA_S = 0.5
KAPPA_Z = 0.05
PAIR_SCALE = 0.02
WIDTH_SQ = 4.0

HIGHEST = lax.Precision.HIGHEST
F32 = jnp.float32
I32 = jnp.int32
VMEM = pl.BlockSpec(memory_space=pltpu.VMEM)
HBM = pl.BlockSpec(memory_space=pltpu.HBM)


def holder_index():
    return lax.axis_index("gy") * 16 + lax.axis_index("gz_0") * 2 + lax.axis_index("gz_1")


def iota(shape, dim):
    return lax.broadcasted_iota(I32, shape, dim)


def shaped(*shape, dtype=F32):
    return jax.ShapeDtypeStruct(shape, dtype)


def call(kernel, out_shape, inputs, **kwargs):
    return pl.pallas_call(
        kernel,
        out_shape=out_shape,
        out_specs=jax.tree.map(lambda _: VMEM, out_shape),
        cost_estimate=pl.CostEstimate(flops=2000000, bytes_accessed=100000, transcendentals=0),
        **kwargs,
    )(*inputs)


def small(kernel, out_shape, inputs, scratch=()):
    return call(
        kernel,
        out_shape,
        inputs,
        in_specs=[VMEM] * len(inputs),
        scratch_shapes=scratch,
        compiler_params=pltpu.CompilerParams(vmem_limit_bytes=8 << 20),
    )


def pair_kernel(pos_ref, aux_ref, xyz_ref, out_ref, select_ref, part_ref, pick_ref):
    columns = [aux_ref[0:2, :].astype(F32), xyz_ref[...], xyz_ref[...]]
    columns = jnp.transpose(jnp.concatenate(columns, axis=0))[0:SLOTS]
    ids = columns[:, 0:1].astype(I32)
    slots = columns[:, 1:2].astype(I32)
    half = lax.axis_index("gz_1") ^ middle(lax.axis_index("gy"))
    source = (ids // BLOCK) ^ TURN ^ half ^ middle(ids // (16 * BLOCK))
    lane = iota((SLOTS, LANES), 1)
    select_ref[...] = (lane == source).astype(F32)
    scale = jnp.where(ids >= 0, -2.0 / P_SIZE, 0.0)
    for c in range(3):
        at = (lane == c * BLOCK + (ids & (BLOCK - 1))).astype(F32)
        whole = jnp.where(lane == 3 * BLOCK, columns[:, c + 2 : c + 3], 0.0)
        part_ref[c * SLOTS : (c + 1) * SLOTS, :] = scale * (whole - at)
    pick_ref[...] = (iota((SLOTS, ATOMS_LOCAL), 1) == slots).astype(F32)
    pos = pos_ref[...]
    columns = jnp.transpose(jnp.concatenate([pos, pos[0:1]] * 2, axis=0))
    scale = -1.0 / (WIDTH_SQ * math.log(2.0))
    step = 64
    sums = [jnp.zeros((8, ATOMS_LOCAL), F32) for _ in range(3)]
    for i in range(0, ATOMS_LOCAL, step):
        diff = [pos[c : c + 1, :] - columns[i : i + step, c : c + 1] for c in range(3)]
        dist_sq = diff[0] * diff[0] + diff[1] * diff[1] + diff[2] * diff[2]
        weight = jnp.exp2(dist_sq * scale)
        for c in range(3):
            term = weight * diff[c]
            for r in range(0, step, 8):
                sums[c] = sums[c] + term[r : r + 8]
    for c in range(3):
        out_ref[c : c + 1, :] = PAIR_SCALE * jnp.sum(sums[c], axis=0, keepdims=True)


def pack_kernel(
    count_hbm, order_hbm, slot_hbm, pos_hbm, rank_hbm, out_ref, aux_ref, xyz_ref, pos_out_ref, count_ref, order_ref, slot_ref, pos_ref, rank_ref, sems
):
    copies = [
        pltpu.make_async_copy(source, target, sems.at[i])
        for i, (source, target) in enumerate(
            (
                (count_hbm, count_ref),
                (order_hbm, order_ref),
                (slot_hbm, slot_ref),
                (pos_hbm, pos_ref),
                (rank_hbm, rank_ref),
            )
        )
    ]
    for copy in copies:
        copy.start()
    here = lax.axis_index("gx") * (2 * N_CHIPS) + holder_index()
    for copy in copies:
        copy.wait()
    counts = count_ref[...]
    domain = iota(counts.shape, 0) * LANES + iota(counts.shape, 1)
    offset = jnp.sum(jnp.where(domain < here, counts, 0))
    mine = jnp.where(domain == here, counts, 0)
    mine = jnp.sum(jnp.sum(mine, axis=0, keepdims=True), axis=1, keepdims=True)
    slots = jnp.concatenate([slot_ref[...]] * 4, axis=1)
    pick = (iota((ATOMS_LOCAL, LANES), 0) == slots).astype(F32)
    pos = pos_ref[...]
    xyz = jnp.dot(pos, pick, precision=HIGHEST, preferred_element_type=F32)
    lane = iota((1, LANES), 1)
    k = lane & (SLOTS - 1)
    live = k < mine
    row = offset // LANES
    shift = offset - row * LANES
    first = order_ref[pl.ds(row, 1), :]
    second = order_ref[pl.ds(jnp.minimum(row + 1, P_SIZE // LANES - 1), 1), :]
    entries = jnp.where(lane >= shift, first, second)
    ids = jnp.full((1, LANES), -1, I32)
    for part in range(4):
        start = shift - part * SLOTS
        turn = jnp.where(start <= 0, -start, LANES - start)
        ids = jnp.where(live & (lane // SLOTS == part), pltpu.roll(entries, turn, 1), ids)
    xyz_ref[...] = xyz
    part = lane // SLOTS
    row_out = jnp.where(part == 0, xyz[0:1], jnp.where(part == 1, xyz[1:2], xyz[2:3]))
    row_out = jnp.where(live, row_out, 0.0)
    row_out = jnp.where(part == 3, ids.astype(F32), row_out)
    out_ref[...] = jnp.broadcast_to(row_out, out_ref.shape)
    aux_ref[...] = jnp.concatenate([ids, slots, rank_ref[...]], axis=0)
    pos_out_ref[...] = pos


def dist_kernel(got_ref, mine_ref, other_ref, out_ref, coded):
    got = got_ref[...]
    part = iota(got.shape, 1) // SLOTS
    ids = jnp.where(part == 3, got, 0.0)
    ids = ids + pltpu.roll(ids, 2 * SLOTS, 1)
    ids = ids + pltpu.roll(ids, SLOTS, 1)
    coded[0] = ids
    coded[1] = jnp.where(part == 3, 1.0, got)
    j = iota((IDS, LANES), 0)
    own = ((holder_index() ^ (j // BLOCK)) * BLOCK + (j & (BLOCK - 1))).astype(F32)
    found = jnp.zeros((IDS, LANES), F32)
    for m in range(N_CHIPS):
        found = found + jnp.where(coded[0, m : m + 1, :] == own, coded[1, m : m + 1, :], 0.0)
    part = iota((IDS, LANES), 1) // SLOTS
    column = [jnp.sum(jnp.where(part == c, found, 0.0), axis=1, keepdims=True) for c in range(4)]
    total = jnp.zeros((BLOCK, F), F32)
    for half, frames_ref in enumerate((mine_ref, other_ref)):
        low = half * BLOCK
        square = jnp.zeros((BLOCK, F), F32)
        for c in range(3):
            delta = column[c][low : low + BLOCK] - frames_ref[c * BLOCK : (c + 1) * BLOCK, :]
            square = square + delta * delta
        total = total + square * column[3][low : low + BLOCK]
    partial = jnp.sum(total, axis=0, keepdims=True) * (1.0 / P_SIZE)
    out_ref[...] = jnp.broadcast_to(partial, out_ref.shape)


def sum_kernel(got_ref, out_ref):
    out_ref[...] = jnp.broadcast_to(jnp.sum(got_ref[...], axis=0, keepdims=True), out_ref.shape)


def bias_kernel(got_ref, aux_ref, mine_ref, other_ref, out_ref, cv_ref):
    dist = jnp.sum(got_ref[...], axis=0, keepdims=True)
    expo = -STRENGTH * dist
    top = jnp.max(expo, axis=1, keepdims=True)
    expd = jnp.exp(expo - top)
    rank = aux_ref[2:3, :].astype(F32) / (F - 1.0)
    total = jnp.sum(expd, axis=1, keepdims=True)
    ranked = jnp.sum(rank * expd, axis=1, keepdims=True)
    s_value = ranked / total
    z_value = -(top + jnp.log(total)) / STRENGTH
    weight = expd / total
    grads = (
        KAPPA_S * P_SIZE * (s_value - S_HOME) * -STRENGTH * weight * (rank - s_value)
        + KAPPA_Z * P_SIZE * z_value * weight
    )
    lane = iota((1, LANES), 1)
    cv_ref[...] = jnp.where(lane == 0, s_value, z_value)
    eight = jnp.broadcast_to(grads, (8, F))
    dims = (((1,), (1,)), ((), ()))
    ones = jnp.ones((BLOCK, F), F32)
    rows = []
    for frames_ref in (mine_ref, other_ref):
        against = jnp.concatenate([frames_ref[...], ones], axis=0)
        sums = lax.dot_general(eight, against, dims, precision=HIGHEST, preferred_element_type=F32)
        rows.append(sums[0:1])
    out_ref[...] = jnp.where((iota(out_ref.shape, 0) & 1) == 0, rows[0], rows[1])


def force_kernel(got_ref, select_ref, part_ref, pick_ref, pair_ref, cv_in_ref, out_ref, cv_ref):
    cv_ref[...] = cv_in_ref[:, 0:2]
    got = got_ref[...]
    high = got.astype(jnp.bfloat16)
    rest = got - high.astype(F32)
    mid = rest.astype(jnp.bfloat16)
    low = (rest - mid.astype(F32)).astype(jnp.bfloat16)
    select = select_ref[...].astype(jnp.bfloat16)
    rows = [jnp.dot(select, piece, preferred_element_type=F32) for piece in (low, mid, high)]
    rows = (rows[0] + rows[1]) + rows[2]
    pick = pick_ref[...]
    for c in range(3):
        part = part_ref[c * SLOTS : (c + 1) * SLOTS, :]
        bias = jnp.sum(rows * part, axis=1, keepdims=True)
        total = jnp.sum(bias * pick, axis=0, keepdims=True)
        out_ref[c : c + 1, :] = pair_ref[c : c + 1, :] + total


def device(x, z, y, core):
    return ((x * 8 + z) * 8 + y) * 2 + core


def chip_groups(first):
    return [
        [
            device(x, z ^ first[0], y ^ first[1], half ^ middle(z ^ first[0]))
            for z in range(8)
            for y in range(8)
        ]
        for x in range(4)
        for half in range(2)
    ]


def first_groups():
    return [
        [device(x, z, y ^ FIRST_FIRST, core ^ 1) for y in range(8) for core in range(2)]
        for x in range(4)
        for z in range(8)
    ]


def second_groups():
    first = SECOND_FIRST
    return [
        [
            device(x ^ first[0], z ^ first[1], y, half ^ middle(z ^ first[1]))
            for x in range(4)
            for z in range(8)
        ]
        for y in range(8)
        for half in range(2)
    ]


def apart(a, b, size):
    return min((a - b) % size, (b - a) % size)


def far_first(groups):
    def hops(a, b):
        a, b = a // 2, b // 2
        x, z, y = (a // 64, b // 64, 4), (a // 8 % 8, b // 8 % 8, 8), (a % 8, b % 8, 8)
        return apart(*x) + apart(*z) + apart(*y)

    return [[g[0]] + sorted(g[1:], key=lambda d: -hops(d, g[0])) for g in groups]


def spread(rows, groups):
    return lax.all_to_all(rows, ALL, 0, 0, tiled=True, axis_index_groups=groups)


def body(positions, frames, path_slot, path_count, path_order, frame_rank):
    mine = jnp.transpose(frames, (1, 2, 0)).reshape(3 * BLOCK, F)
    other = lax.ppermute(mine, "gz_1", [(0, 1), (1, 0)])
    inputs = (
        path_count.reshape(4, LANES),
        path_order.reshape(32, LANES),
        path_slot,
        positions,
        frame_rank.reshape(1, F),
    )
    inputs = tuple(pltpu.with_memory_space_constraint(a, pltpu.HBM) for a in inputs)
    sent, aux, xyz, pos = call(
        pack_kernel,
        (
            shaped(N_CHIPS, LANES),
            shaped(3, LANES, dtype=I32),
            shaped(3, LANES),
            shaped(3, ATOMS_LOCAL),
        ),
        inputs,
        in_specs=[HBM] * len(inputs),
        scratch_shapes=[pltpu.VMEM(a.shape, a.dtype) for a in inputs]
        + [pltpu.SemaphoreType.DMA((len(inputs),))],
        compiler_params=pltpu.CompilerParams(vmem_limit_bytes=8 << 20),
    )
    atoms = spread(sent, far_first(chip_groups(ATOMS_FIRST)))
    coded = [pltpu.VMEM((2, N_CHIPS, LANES), F32)]
    partial = small(dist_kernel, shaped(N_FIRST, LANES), (atoms, mine, other), coded)
    first = spread(partial, far_first(first_groups()))
    row_sum = small(sum_kernel, shaped(N_SECOND, LANES), (first,))
    second = spread(row_sum, far_first(second_groups()))
    biases, cv = small(
        bias_kernel, (shaped(2 * N_CHIPS, LANES), shaped(1, LANES)), (second, aux, mine, other)
    )
    back = spread(biases, chip_groups(BIAS_FIRST))
    pair, select, part, pick = small(
        pair_kernel,
        (
            shaped(3, ATOMS_LOCAL),
            shaped(SLOTS, LANES),
            shaped(3 * SLOTS, LANES),
            shaped(SLOTS, ATOMS_LOCAL),
        ),
        (pos, aux, xyz),
    )
    forces, cv = small(
        force_kernel, (shaped(3, ATOMS_LOCAL), shaped(1, 2)), (back, select, part, pick, pair, cv)
    )
    return forces, cv.reshape(2)


def solution(mesh):
    finer = Mesh(mesh.devices.reshape(mesh.shape["gx"], mesh.shape["gy"], 8, 2), ALL)
    return jax.shard_map(
        body,
        mesh=finer,
        in_specs=(P(None, ALL), P(None, None, HOLDERS), P(ALL, None), P(), P(), P()),
        out_specs=(P(None, ALL), P()),
        check_vma=False,
    )
```

```python
import math

import jax
import jax.numpy as jnp
from jax import lax
from jax.experimental import pallas as pl
from jax.experimental.pallas import tpu as pltpu
from jax.sharding import Mesh
from jax.sharding import PartitionSpec as P


P_SIZE = 4096
F = 128
ATOMS_LOCAL = 512
SLOTS = 32
LANES = 128
BLOCK = 32

ALL = ("gx", "gy", "gz_0", "gz_1")
HOLDERS = ("gy", "gz_0", "gz_1")
N_CHIPS = 64
IDS = 2 * BLOCK
N_FIRST = 16
N_SECOND = 32

ATOMS_FIRST = (5, 5)
FIRST_FIRST = 4
SECOND_FIRST = (2, 5)
BIAS_FIRST = (4, 4)
TURN = 16 * BIAS_FIRST[0] + 2 * BIAS_FIRST[1]


def middle(z):
    return ((z + 2) & 4) // 4


STRENGTH = 20.0
S_HOME = 0.5
KAPPA_S = 0.5
KAPPA_Z = 0.05
PAIR_SCALE = 0.02
WIDTH_SQ = 4.0

HIGHEST = lax.Precision.HIGHEST
F32 = jnp.float32
I32 = jnp.int32
VMEM = pl.BlockSpec(memory_space=pltpu.VMEM)
HBM = pl.BlockSpec(memory_space=pltpu.HBM)


def holder_index():
    return lax.axis_index("gy") * 16 + lax.axis_index("gz_0") * 2 + lax.axis_index("gz_1")


def iota(shape, dim):
    return lax.broadcasted_iota(I32, shape, dim)


def shaped(*shape, dtype=F32):
    return jax.ShapeDtypeStruct(shape, dtype)


def call(kernel, out_shape, inputs, **kwargs):
    return pl.pallas_call(
        kernel,
        out_shape=out_shape,
        out_specs=jax.tree.map(lambda _: VMEM, out_shape),
        cost_estimate=pl.CostEstimate(flops=2000000, bytes_accessed=100000, transcendentals=0),
        **kwargs,
    )(*inputs)


def small(kernel, out_shape, inputs, scratch=()):
    return call(
        kernel,
        out_shape,
        inputs,
        in_specs=[VMEM] * len(inputs),
        scratch_shapes=scratch,
        compiler_params=pltpu.CompilerParams(vmem_limit_bytes=8 << 20),
    )


def pair_kernel(pos_ref, aux_ref, xyz_ref, out_ref, select_ref, part_ref, pick_ref):
    columns = [aux_ref[0:2, :].astype(F32), xyz_ref[...], xyz_ref[...]]
    columns = jnp.transpose(jnp.concatenate(columns, axis=0))[0:SLOTS]
    ids = columns[:, 0:1].astype(I32)
    slots = columns[:, 1:2].astype(I32)
    half = lax.axis_index("gz_1") ^ middle(lax.axis_index("gy"))
    source = (ids // BLOCK) ^ TURN ^ half ^ middle(ids // (16 * BLOCK))
    lane = iota((SLOTS, LANES), 1)
    select_ref[...] = (lane == source).astype(F32)
    scale = jnp.where(ids >= 0, -2.0 / P_SIZE, 0.0)
    for c in range(3):
        at = (lane == c * BLOCK + (ids & (BLOCK - 1))).astype(F32)
        whole = jnp.where(lane == 3 * BLOCK, columns[:, c + 2 : c + 3], 0.0)
        part_ref[c * SLOTS : (c + 1) * SLOTS, :] = scale * (whole - at)
    pick_ref[...] = (iota((SLOTS, ATOMS_LOCAL), 1) == slots).astype(F32)
    pos = pos_ref[...]
    columns = jnp.transpose(jnp.concatenate([pos, pos[0:1]] * 2, axis=0))
    scale = -1.0 / (WIDTH_SQ * math.log(2.0))
    step = 64
    sums = [jnp.zeros((8, ATOMS_LOCAL), F32) for _ in range(3)]
    for i in range(0, ATOMS_LOCAL, step):
        diff = [pos[c : c + 1, :] - columns[i : i + step, c : c + 1] for c in range(3)]
        dist_sq = diff[0] * diff[0] + diff[1] * diff[1] + diff[2] * diff[2]
        weight = jnp.exp2(dist_sq * scale)
        for c in range(3):
            term = weight * diff[c]
            for r in range(0, step, 8):
                sums[c] = sums[c] + term[r : r + 8]
    for c in range(3):
        out_ref[c : c + 1, :] = PAIR_SCALE * jnp.sum(sums[c], axis=0, keepdims=True)


def pack_kernel(
    count_hbm, order_hbm, slot_hbm, pos_hbm, rank_hbm, out_ref, aux_ref, xyz_ref, pos_out_ref, count_ref, order_ref, slot_ref, pos_ref, rank_ref, sems
):
    copies = [
        pltpu.make_async_copy(source, target, sems.at[i])
        for i, (source, target) in enumerate(
            (
                (count_hbm, count_ref),
                (order_hbm, order_ref),
                (slot_hbm, slot_ref),
                (pos_hbm, pos_ref),
                (rank_hbm, rank_ref),
            )
        )
    ]
    for copy in copies:
        copy.start()
    here = lax.axis_index("gx") * (2 * N_CHIPS) + holder_index()
    for copy in copies:
        copy.wait()
    counts = count_ref[...]
    domain = iota(counts.shape, 0) * LANES + iota(counts.shape, 1)
    offset = jnp.sum(jnp.where(domain < here, counts, 0))
    mine = jnp.where(domain == here, counts, 0)
    mine = jnp.sum(jnp.sum(mine, axis=0, keepdims=True), axis=1, keepdims=True)
    slots = jnp.concatenate([slot_ref[...]] * 4, axis=1)
    pick = (iota((ATOMS_LOCAL, LANES), 0) == slots).astype(F32)
    pos = pos_ref[...]
    xyz = jnp.dot(pos, pick, precision=HIGHEST, preferred_element_type=F32)
    lane = iota((1, LANES), 1)
    k = lane & (SLOTS - 1)
    live = k < mine
    row = offset // LANES
    shift = offset - row * LANES
    first = order_ref[pl.ds(row, 1), :]
    second = order_ref[pl.ds(jnp.minimum(row + 1, P_SIZE // LANES - 1), 1), :]
    entries = jnp.where(lane >= shift, first, second)
    ids = jnp.full((1, LANES), -1, I32)
    for part in range(4):
        start = shift - part * SLOTS
        turn = jnp.where(start <= 0, -start, LANES - start)
        ids = jnp.where(live & (lane // SLOTS == part), pltpu.roll(entries, turn, 1), ids)
    xyz_ref[...] = xyz
    part = lane // SLOTS
    row_out = jnp.where(part == 0, xyz[0:1], jnp.where(part == 1, xyz[1:2], xyz[2:3]))
    row_out = jnp.where(live, row_out, 0.0)
    row_out = jnp.where(part == 3, ids.astype(F32), row_out)
    out_ref[...] = jnp.broadcast_to(row_out, out_ref.shape)
    aux_ref[...] = jnp.concatenate([ids, slots, rank_ref[...]], axis=0)
    pos_out_ref[...] = pos


def dist_kernel(got_ref, mine_ref, other_ref, out_ref, coded):
    got = got_ref[...]
    part = iota(got.shape, 1) // SLOTS
    ids = jnp.where(part == 3, got, 0.0)
    ids = ids + pltpu.roll(ids, 2 * SLOTS, 1)
    ids = ids + pltpu.roll(ids, SLOTS, 1)
    coded[0] = ids
    coded[1] = jnp.where(part == 3, 1.0, got)
    j = iota((IDS, LANES), 0)
    own = ((holder_index() ^ (j // BLOCK)) * BLOCK + (j & (BLOCK - 1))).astype(F32)
    found = jnp.zeros((IDS, LANES), F32)
    for m in range(N_CHIPS):
        found = found + jnp.where(coded[0, m : m + 1, :] == own, coded[1, m : m + 1, :], 0.0)
    part = iota((IDS, LANES), 1) // SLOTS
    column = [jnp.sum(jnp.where(part == c, found, 0.0), axis=1, keepdims=True) for c in range(4)]
    total = jnp.zeros((BLOCK, F), F32)
    for half, frames_ref in enumerate((mine_ref, other_ref)):
        low = half * BLOCK
        square = jnp.zeros((BLOCK, F), F32)
        for c in range(3):
            delta = column[c][low : low + BLOCK] - frames_ref[c * BLOCK : (c + 1) * BLOCK, :]
            square = square + delta * delta
        total = total + square * column[3][low : low + BLOCK]
    partial = jnp.sum(total, axis=0, keepdims=True) * (1.0 / P_SIZE)
    out_ref[...] = jnp.broadcast_to(partial, out_ref.shape)


def sum_kernel(got_ref, out_ref):
    out_ref[...] = jnp.broadcast_to(jnp.sum(got_ref[...], axis=0, keepdims=True), out_ref.shape)


def bias_kernel(got_ref, aux_ref, mine_ref, other_ref, out_ref, cv_ref):
    dist = jnp.sum(got_ref[...], axis=0, keepdims=True)
    expo = -STRENGTH * dist
    top = jnp.max(expo, axis=1, keepdims=True)
    expd = jnp.exp(expo - top)
    rank = aux_ref[2:3, :].astype(F32) / (F - 1.0)
    total = jnp.sum(expd, axis=1, keepdims=True)
    ranked = jnp.sum(rank * expd, axis=1, keepdims=True)
    s_value = ranked / total
    z_value = -(top + jnp.log(total)) / STRENGTH
    weight = expd / total
    grads = (
        KAPPA_S * P_SIZE * (s_value - S_HOME) * -STRENGTH * weight * (rank - s_value)
        + KAPPA_Z * P_SIZE * z_value * weight
    )
    lane = iota((1, LANES), 1)
    cv_ref[...] = jnp.where(lane == 0, s_value, z_value)
    eight = jnp.broadcast_to(grads, (8, F))
    dims = (((1,), (1,)), ((), ()))
    ones = jnp.ones((BLOCK, F), F32)
    rows = []
    for frames_ref in (mine_ref, other_ref):
        against = jnp.concatenate([frames_ref[...], ones], axis=0)
        sums = lax.dot_general(eight, against, dims, precision=HIGHEST, preferred_element_type=F32)
        rows.append(sums[0:1])
    out_ref[...] = jnp.where((iota(out_ref.shape, 0) & 1) == 0, rows[0], rows[1])


def force_kernel(got_ref, select_ref, part_ref, pick_ref, pair_ref, cv_in_ref, out_ref, cv_ref):
    cv_ref[...] = cv_in_ref[:, 0:2]
    got = got_ref[...]
    high = got.astype(jnp.bfloat16)
    rest = got - high.astype(F32)
    mid = rest.astype(jnp.bfloat16)
    low = (rest - mid.astype(F32)).astype(jnp.bfloat16)
    select = select_ref[...].astype(jnp.bfloat16)
    rows = [jnp.dot(select, piece, preferred_element_type=F32) for piece in (low, mid, high)]
    rows = (rows[0] + rows[1]) + rows[2]
    pick = pick_ref[...]
    for c in range(3):
        part = part_ref[c * SLOTS : (c + 1) * SLOTS, :]
        bias = jnp.sum(rows * part, axis=1, keepdims=True)
        total = jnp.sum(bias * pick, axis=0, keepdims=True)
        out_ref[c : c + 1, :] = pair_ref[c : c + 1, :] + total


def device(x, z, y, core):
    return ((x * 8 + z) * 8 + y) * 2 + core


def chip_groups(first):
    return [
        [
            device(x, z ^ first[0], y ^ first[1], half ^ middle(z ^ first[0]))
            for z in range(8)
            for y in range(8)
        ]
        for x in range(4)
        for half in range(2)
    ]


def first_groups():
    return [
        [device(x, z, y ^ FIRST_FIRST, core ^ 1) for y in range(8) for core in range(2)]
        for x in range(4)
        for z in range(8)
    ]


def second_groups():
    first = SECOND_FIRST
    return [
        [
            device(x ^ first[0], z ^ first[1], y, half ^ middle(z ^ first[1]))
            for x in range(4)
            for z in range(8)
        ]
        for y in range(8)
        for half in range(2)
    ]


def spread(rows, groups):
    return lax.all_to_all(rows, ALL, 0, 0, tiled=True, axis_index_groups=groups)


def body(positions, frames, path_slot, path_count, path_order, frame_rank):
    mine = jnp.transpose(frames, (1, 2, 0)).reshape(3 * BLOCK, F)
    other = lax.ppermute(mine, "gz_1", [(0, 1), (1, 0)])
    inputs = (
        path_count.reshape(4, LANES),
        path_order.reshape(32, LANES),
        path_slot,
        positions,
        frame_rank.reshape(1, F),
    )
    inputs = tuple(pltpu.with_memory_space_constraint(a, pltpu.HBM) for a in inputs)
    sent, aux, xyz, pos = call(
        pack_kernel,
        (
            shaped(N_CHIPS, LANES),
            shaped(3, LANES, dtype=I32),
            shaped(3, LANES),
            shaped(3, ATOMS_LOCAL),
        ),
        inputs,
        in_specs=[HBM] * len(inputs),
        scratch_shapes=[pltpu.VMEM(a.shape, a.dtype) for a in inputs]
        + [pltpu.SemaphoreType.DMA((len(inputs),))],
        compiler_params=pltpu.CompilerParams(vmem_limit_bytes=8 << 20),
    )
    atoms = spread(sent, chip_groups(ATOMS_FIRST))
    coded = [pltpu.VMEM((2, N_CHIPS, LANES), F32)]
    partial = small(dist_kernel, shaped(N_FIRST, LANES), (atoms, mine, other), coded)
    first = spread(partial, first_groups())
    row_sum = small(sum_kernel, shaped(N_SECOND, LANES), (first,))
    second = spread(row_sum, second_groups())
    biases, cv = small(
        bias_kernel, (shaped(2 * N_CHIPS, LANES), shaped(1, LANES)), (second, aux, mine, other)
    )
    back = spread(biases, chip_groups(BIAS_FIRST))
    pair, select, part, pick = small(
        pair_kernel,
        (
            shaped(3, ATOMS_LOCAL),
            shaped(SLOTS, LANES),
            shaped(3 * SLOTS, LANES),
            shaped(SLOTS, ATOMS_LOCAL),
        ),
        (pos, aux, xyz),
    )
    forces, cv = small(
        force_kernel, (shaped(3, ATOMS_LOCAL), shaped(1, 2)), (back, select, part, pick, pair, cv)
    )
    return forces, cv.reshape(2)


def solution(mesh):
    finer = Mesh(mesh.devices.reshape(mesh.shape["gx"], mesh.shape["gy"], 8, 2), ALL)
    return jax.shard_map(
        body,
        mesh=finer,
        in_specs=(P(None, ALL), P(None, None, HOLDERS), P(ALL, None), P(), P(), P()),
        out_specs=(P(None, ALL), P()),
        check_vma=False,
    )
```
